32 devices in a mesh: group: 2 (over x), expert: 8 (over z, y), dp: 2 (over core).
Axes of the slice: x: 2, y: 2, z: 4, core: 2. Of those that a mesh axis runs over, the one named last changes fastest.
Arguments:
- tokens: bfloat16 [4096, 2048], P(('group', 'expert', 'dp')), parts along dimension 0, may hold values from -30 to 30
- expert_choice: int32 [4096, 2], P(('group', 'expert', 'dp')), parts along dimension 0, may hold values from 0 to 3, all different within a row; in each aligned block of 128 rows (0 to 127, 128 to 255, ...) at most 70 rows name the same one
- gate_weights: float32 [4096, 2], P(('group', 'expert', 'dp')), parts along dimension 0, may hold values from 0.1 to 1
- attention_gain: float32 [2048], replicated, may hold values from 0.1 to 1.9
- query_weight: bfloat16 [2048, 2048], P('dp'), may hold values from -0.13258252 to 0.13258252
- key_value_weight: bfloat16 [2048, 1024], P('dp'), may hold values from -3.2040776022515436 to 3.2040776022515436
- output_weight: bfloat16 [2048, 2048], P('dp'), may hold values from -0.125 to 0.125
- feedforward_gain: float32 [2048], replicated, may hold values from 0.1 to 1.9
- expert_gate: bfloat16 [2048, 28672], P(None, ('expert', 'dp')), may hold values from -0.125 to 0.125
- expert_up: bfloat16 [2048, 28672], P(None, ('expert', 'dp')), may hold values from -0.125 to 0.125
- expert_down: bfloat16 [28672, 2048], P(('expert', 'dp')), may hold values from -0.0625 to 0.0625
Outputs:
- layer_output: bfloat16 [4096, 2048], P(('group', 'expert', 'dp')), parts along dimension 0
The draws below stay inside these ranges and needn't reach their ends.
There are 2 independent parts, one for each index of `group`. The reference program is written for one: setup_inputs(seed, part) draws one part's arguments, and reference() takes and returns one part's arrays. A program takes and returns all parts, laid end to end along the dimension named above; an argument that names none is the same for every part. Nothing has to cross between parts.
Inputs may be any that keep to these rules, and one draw needn't show every extreme that they name: `expert_choice`: each row names 2 different experts; within the rows of one device no expert is named more than 70 times, and some device's expert is named exactly 70 times.
All inputs are finite; a program needn't handle non-finite values.
Results may differ from the reference program's by a relative error of at most 0.012.
Values may be sent and summed in bfloat16 or wider, within the bound.
No kernel may reach another device: no remote copies, remote signals or barrier semaphores. Data moves between devices by JAX's collectives and lax.ppermute only.
A program may use at most 128 MiB of HBM per device.

```python
import math
import jax
import jax.numpy as jnp
import numpy as np
from jax import lax

D = 2048
HEADS = 16
KV_HEADS = 4
HEAD_DIM = 128
EXPERTS = 4
FF = 7168
TOP = 2
TOK_DEV = 128
CAP = 70
LENGTH = 2048
QW = 2048
N_EXPERT = 8
N_DP = 2


def paired_weights(key):
    first, second = jax.random.split(jax.random.fold_in(key, 4177))
    scale = D ** (-0.5)
    query = jnp.clip(jax.random.normal(first, (D, HEADS * HEAD_DIM), jnp.float32), -6.0, 6.0) * scale
    keyval = jnp.clip(jax.random.normal(second, (D, 2 * KV_HEADS * HEAD_DIM), jnp.float32), -6.0, 6.0) * scale
    return (query, keyval)


def draw_query_weight(key, part):
    return paired_weights(key)[0].astype(jnp.bfloat16)


def draw_key_value_weight(key, part):
    return paired_weights(key)[1].astype(jnp.bfloat16)


def draw_tokens(key, part):
    first = jax.random.fold_in(jax.random.fold_in(key, 911), 0)
    values = jnp.clip(jax.random.normal(first, (LENGTH, D), jnp.float32), -6.0, 6.0)
    return values.astype(jnp.bfloat16)


def steps_of(stream_key, extent, cuts, smallest, high):
    loudness, own = 1.0, jax.random.fold_in(stream_key, 6)
    for position, shards_of in cuts:
        draws = jnp.exp(jax.random.uniform(jax.random.fold_in(own, position), (shards_of,), jnp.float32, smallest / len(cuts), high / len(cuts)))
        loudness = loudness * jnp.repeat(draws, extent[position] // shards_of).reshape([-1 if axis == position else 1 for axis in range(len(extent))])
    return loudness


def routed_block(own_key, own, number, rows, amount, top, most, lean):
    order = jax.random.permutation(own_key, amount)
    crowded, usual = load_shares(amount, rows * top, most, lean, True), load_shares(amount, rows * top, most, lean, False)
    places = jnp.arange(amount)

    def named(lengths, rotation):
        used = int((lengths > 0).sum())
        fixed = max(1, used // 4)
        passed = fixed + (places - fixed + rotation * (used - fixed)) % max(1, amount - fixed)
        return jnp.zeros((amount,), jnp.int32).at[order[jnp.where(places < fixed, places, passed)]].set(jnp.asarray(lengths, jnp.int32))

    lengths = jnp.where(number % 4 == 0, named(crowded, number // 4), named(usual, number - number // 4 - 1))
    mixed = jax.random.permutation(jax.random.fold_in(own, 3), amount)
    giver, sink = mixed[0:amount // 2 * 2:2], mixed[1:amount // 2 * 2:2]
    margin = jnp.minimum(lengths[giver] - 1, most - lengths[sink]) // 2
    margin = jnp.where((giver == order[0]) | (sink == order[0]) | (lengths[sink] == 0), 0, jnp.maximum(margin, 0))
    passed = jax.random.randint(jax.random.fold_in(own, 4), (amount // 2,), 0, 1 << 20) % (margin + 1)
    lengths = lengths.at[giver].add(-passed).at[sink].add(passed)
    members = jnp.searchsorted(jnp.cumsum(lengths), jnp.arange(rows * top), side="right").astype(jnp.int32)
    listing = members.reshape(top, rows).T
    listing = listing[jax.random.permutation(jax.random.fold_in(own, 1), rows)]
    rotation = jax.random.randint(jax.random.fold_in(own, 2), (rows, 1), 0, top)
    return jnp.take_along_axis(listing, (jnp.arange(top)[None, :] + rotation) % top, axis=1)


def load_shares(number_of, total, reach, lean, full):
    weights = [(1 << 20) // math.isqrt(standing ** lean) + 1 for standing in range(1, number_of + 1)]
    largest = reach if full else min(reach, max(-(-total // number_of), total * weights[0] // sum(weights)))
    least = 1 if total - largest >= number_of - 1 else 0
    holding, rest = [largest] + [least] * (number_of - 1), total - largest - least * (number_of - 1)
    while rest > 0:
        movable = [i for i in range(1, number_of) if holding[i] < largest] or [i for i in range(1, number_of) if holding[i] < reach]
        whole, left = sum([weights[i] for i in movable]), rest
        for i in movable:
            more = min(reach - holding[i], max(1, left * weights[i] // whole), rest)
            holding[i] = holding[i] + more
            rest = rest - more
    return np.array(holding)


def normal_values(stream_key, extent, scale, most, cuts=(), kind=jnp.bfloat16):
    entries = scale * jax.random.normal(stream_key, extent, jnp.float32)
    if cuts:
        entries = entries * steps_of(stream_key, extent, cuts, -0.22, 0.18)
    return jnp.clip(entries, -most, most).astype(kind)


def setup_inputs(seed: int = 0, part: int = 0) -> dict:
    arg_keys = jax.random.split(jax.random.key(seed), 12)
    own_keys = jax.random.split(jax.random.fold_in(arg_keys[11], part), 12)
    tokens = draw_tokens(jax.random.fold_in(jax.random.fold_in(arg_keys[11], part), 71), part)
    expert_choice_keys = jax.random.split(jax.random.fold_in(own_keys[1], 1), LENGTH // TOK_DEV)
    expert_choice_turns = jax.random.permutation(jax.random.fold_in(own_keys[1], 3), LENGTH // TOK_DEV)
    expert_choice = jax.vmap(lambda own, number: routed_block(jax.random.fold_in(own_keys[1], 2), own, number, TOK_DEV, EXPERTS, TOP, CAP, 1))(expert_choice_keys, expert_choice_turns).reshape((LENGTH, TOP))
    gate_weights = jnp.clip(0.1 + 0.9 * jax.random.uniform(own_keys[2], (LENGTH, TOP), jnp.float32) ** steps_of(own_keys[2], (LENGTH, TOP), ((0, 16),), -0.2, 0.2), 0.1, 1.0)
    attention_gain = jnp.clip(1.0 + 0.18 * jax.random.normal(arg_keys[3], (D,), jnp.float32), 0.1, 1.9)
    query_weight = draw_query_weight(jax.random.fold_in(arg_keys[11], 71), part)
    key_value_weight = draw_key_value_weight(jax.random.fold_in(arg_keys[11], 71), part)
    output_weight = normal_values(arg_keys[6], (QW, D), QW ** -0.5, 0.125, ((0, 2),))
    feedforward_gain = jnp.clip(1.0 + 0.18 * jax.random.normal(arg_keys[7], (D,), jnp.float32), 0.1, 1.9)
    expert_gate = normal_values(arg_keys[8], (D, EXPERTS * FF), D ** -0.5, 0.125, ((1, 16),))
    expert_up = normal_values(arg_keys[9], (D, EXPERTS * FF), D ** -0.5, 0.125, ((1, 16),))
    expert_down = normal_values(arg_keys[10], (EXPERTS * FF, D), FF ** -0.5, 0.0625, ((0, 16),))
    return dict(tokens=tokens, expert_choice=expert_choice, gate_weights=gate_weights, attention_gain=attention_gain, query_weight=query_weight, key_value_weight=key_value_weight, output_weight=output_weight, feedforward_gain=feedforward_gain, expert_gate=expert_gate, expert_up=expert_up, expert_down=expert_down)


epsilon = 1e-05
base_theta = 1000000.0
masked_score = -1e+30

def rms_norm(values, gain):
    widened = values.astype(jnp.float32)
    spread = lax.optimization_barrier(jnp.mean(widened * widened, axis=-1, keepdims=True))
    return (widened * lax.rsqrt(spread + epsilon) * gain).astype(jnp.bfloat16)

def rotary(vectors, positions):
    halfway = vectors.shape[-1] // 2
    powers = jnp.arange(halfway, dtype=jnp.float32) * (2.0 / vectors.shape[-1])
    inverse = base_theta ** (-powers)
    angles = positions.astype(jnp.float32)[:, None] * inverse[None, :]
    cosine = jnp.cos(angles)[:, None, :]
    sine = jnp.sin(angles)[:, None, :]
    former = vectors[..., :halfway]
    latter = vectors[..., halfway:]
    return jnp.concatenate([former * cosine - latter * sine, latter * cosine + former * sine], axis=-1)

def reference(tokens, expert_choice, gate_weights, attention_gain, query_weight, key_value_weight, output_weight, feedforward_gain, expert_gate, expert_up, expert_down):
    length = tokens.shape[0]
    key_width = KV_HEADS * HEAD_DIM
    sharing = HEADS // KV_HEADS
    normed = rms_norm(tokens, attention_gain)
    query_raw = jnp.dot(normed, query_weight, preferred_element_type=jnp.float32)
    keyval_raw = jnp.dot(normed, key_value_weight, preferred_element_type=jnp.float32)
    positions = jnp.arange(length, dtype=jnp.int32)
    queries = rotary(query_raw.reshape(length, HEADS, HEAD_DIM), positions).astype(jnp.bfloat16)
    keys = rotary(keyval_raw[:, :key_width].reshape(length, KV_HEADS, HEAD_DIM), positions).astype(jnp.bfloat16)
    values = keyval_raw[:, key_width:].reshape(length, KV_HEADS, HEAD_DIM).astype(jnp.bfloat16)
    block = min(512, length)
    query_blocks = queries.reshape(length // block, block, KV_HEADS, sharing, HEAD_DIM)
    position_blocks = positions.reshape(length // block, block)
    scale = HEAD_DIM ** (-0.5)
    key_positions = jnp.arange(length, dtype=jnp.int32)

    def attend(operands):
        query_block, query_positions = operands
        scores = jnp.einsum('qcgd,kcd->cgqk', query_block.astype(jnp.float32), keys.astype(jnp.float32)) * scale
        visible = key_positions[None, :] <= query_positions[:, None]
        scores = jnp.where(visible, scores, masked_score)
        highest = lax.optimization_barrier(jnp.max(scores, axis=-1, keepdims=True))
        expo = jnp.where(visible, jnp.exp(scores - highest), 0.0)
        totals = lax.optimization_barrier(jnp.sum(expo, axis=-1))
        probs = expo.astype(jnp.bfloat16)
        mixed = jnp.einsum('cgqk,kcd->qcgd', probs.astype(jnp.float32), values.astype(jnp.float32))
        mixed = mixed / jnp.transpose(totals, (2, 0, 1))[..., None]
        return mixed.reshape(block, HEADS * HEAD_DIM).astype(jnp.bfloat16)
    context = lax.map(attend, (query_blocks, position_blocks)).reshape(length, HEADS * HEAD_DIM)
    attention = jnp.dot(context, output_weight, preferred_element_type=jnp.float32)
    residual = (tokens.astype(jnp.float32) + attention).astype(jnp.bfloat16)
    mixed_in = rms_norm(residual, feedforward_gain)
    slabs = N_EXPERT * N_DP // EXPERTS
    slab_width = FF // slabs
    mixture = jnp.zeros((length, D), jnp.float32)
    for expert in range(EXPERTS):
        weight = lax.optimization_barrier(jnp.sum(jnp.where(expert_choice == expert, gate_weights, jnp.zeros_like(gate_weights)), axis=1))
        lowest = expert * FF
        gate = jnp.dot(mixed_in, expert_gate[:, lowest:lowest + FF], preferred_element_type=jnp.float32)
        upward = jnp.dot(mixed_in, expert_up[:, lowest:lowest + FF], preferred_element_type=jnp.float32)
        hidden = (jax.nn.silu(gate) * upward).astype(jnp.bfloat16)
        summed = jnp.zeros((length, D), jnp.float32)
        for slab in range(slabs):
            first_row = lowest + slab * slab_width
            term = jnp.dot(hidden[:, slab * slab_width:(slab + 1) * slab_width], expert_down[first_row:first_row + slab_width], preferred_element_type=jnp.float32).astype(jnp.bfloat16)
            summed = summed + lax.optimization_barrier(term).astype(jnp.float32)
        mixture = mixture + weight[:, None] * summed
    return (residual.astype(jnp.float32) + mixture).astype(jnp.bfloat16)
```

```python
import functools
import math

import jax
import jax.numpy as jnp
from jax import lax
from jax.experimental import pallas as pl
from jax.experimental.pallas import tpu as pltpu
from jax.sharding import PartitionSpec as P

HEAD_DIM = 128
EXPERTS = 4
TOP = 2
CAP = 70
ROWS = -(-CAP // 8) * 8

epsilon = 1e-05
base_theta = 1000000.0
masked_score = -1e30

VMEM = pl.BlockSpec(memory_space=pltpu.VMEM)
f32 = jnp.float32
bf16 = jnp.bfloat16


def dot(a, b):
    return jnp.dot(a, b, preferred_element_type=f32)


def call(kernel, outs, operands, scratch=(), flops=0, moved=0, limit=24 << 20, name=None):
    return pl.pallas_call(
        kernel,
        out_shape=outs,
        in_specs=[VMEM] * len(operands),
        out_specs=jax.tree.map(lambda _: VMEM, outs),
        scratch_shapes=list(scratch),
        compiler_params=pltpu.CompilerParams(vmem_limit_bytes=limit),
        cost_estimate=pl.CostEstimate(flops=flops, bytes_accessed=moved, transcendentals=0),
        name=name,
    )(*operands)


def normalized(widened, gain):
    spread = jnp.mean(widened * widened, axis=-1, keepdims=True)
    return (widened * lax.rsqrt(spread + epsilon) * gain).astype(bf16)


def norm_kernel(tokens_ref, gain_ref, keep_ref, send_ref, whole_ref):
    half = keep_ref.shape[1]
    whole_ref[...] = normalized(tokens_ref[...].astype(f32), gain_ref[...])
    core = lax.axis_index("dp")
    keep_ref[...] = whole_ref[:, pl.ds(pl.multiple_of(core * half, half), half)]
    send_ref[...] = whole_ref[:, pl.ds(pl.multiple_of((1 - core) * half, half), half)]


def keyval_kernel(mine_ref, theirs_ref, weight_ref, keep_ref, send_ref):
    rows = jnp.concatenate([mine_ref[...], theirs_ref[...]], axis=0)
    width = keep_ref.shape[1] // 2
    core = lax.axis_index("dp")
    for out_ref, owner in ((send_ref, 1 - core), (keep_ref, core)):
        for part in range(2):
            start = pl.multiple_of((part * 2 + owner) * width, width)
            out_ref[:, part * width : (part + 1) * width] = dot(
                rows, weight_ref[:, pl.ds(start, width)]
            )


def query_kernel(mine_ref, theirs_ref, weight_ref, keep_ref, send_ref):
    rows = jnp.concatenate([mine_ref[...], theirs_ref[...]], axis=0)
    width = keep_ref.shape[1]
    step = min(512, width)
    core = lax.axis_index("dp")
    for out_ref, owner in ((send_ref, 1 - core), (keep_ref, core)):
        for offset in range(0, width, step):
            start = pl.multiple_of(owner * width + offset, step)
            out_ref[:, offset : offset + step] = dot(rows, weight_ref[:, pl.ds(start, step)])


def summed(keep_ref, came_ref, columns):
    half = keep_ref.shape[0] // 2
    came = came_ref[:, columns]
    return keep_ref[:, columns] + jnp.concatenate([came[half:], came[:half]], axis=0)


def turned(vectors, cosine, sine):
    return vectors * cosine + pltpu.roll(vectors, HEAD_DIM // 2, 1) * sine


def keyval_turn_kernel(keep_ref, came_ref, cosine_ref, sine_ref, out_ref):
    width = out_ref.shape[1]
    for start in range(0, width, HEAD_DIM):
        columns = slice(start, start + HEAD_DIM)
        total = summed(keep_ref, came_ref, columns)
        if start < width // 2:
            total = turned(total, cosine_ref[...], sine_ref[...])
        out_ref[:, columns] = total.astype(bf16)


def query_turn_kernel(keep_ref, came_ref, cosine_ref, sine_ref, out_ref):
    for head in range(out_ref.shape[0]):
        columns = slice(head * HEAD_DIM, (head + 1) * HEAD_DIM)
        total = summed(keep_ref, came_ref, columns)
        out_ref[head] = turned(total, cosine_ref[...], sine_ref[...]).astype(bf16)


def attention_kernel(places, along, query_ref, weight_ref, *refs):
    keyval_refs = refs[: len(places)]
    send_ref, keep_ref, score_ref, context_ref = refs[len(places) :]
    heads, rows, _ = query_ref.shape
    half = rows // 2
    shared = keyval_refs[0].shape[1] // (2 * HEAD_DIM)
    sharing = heads // shared
    core = lax.axis_index("dp")
    chip = lax.axis_index("expert")
    plane, place = chip // along, chip % along

    def position(shape, axis):
        row = lax.broadcasted_iota(jnp.int32, shape, axis)
        return jnp.where(core == 0, row, jnp.where(row < half, row + half, row - half))

    own_visible = position((rows, rows), 1) <= position((rows, rows), 0)
    seen = []
    for back, turn in places:
        if back == 0:
            seen.append((place ^ turn) < place)
        else:
            seen.append(plane >= back)
    factor = HEAD_DIM ** (-0.5) * math.log2(math.e)

    for group in range(shared):
        key_columns = slice(group * HEAD_DIM, (group + 1) * HEAD_DIM)
        value_columns = slice((shared + group) * HEAD_DIM, (shared + group + 1) * HEAD_DIM)

        def one_head(member, _):
            head = group * sharing + member
            query = query_ref[head]
            highest = jnp.full((rows, HEAD_DIM), masked_score, f32)
            for index, keyval_ref in enumerate(keyval_refs):
                score = lax.dot_general(
                    query,
                    keyval_ref[:, key_columns],
                    (((1,), (1,)), ((), ())),
                    preferred_element_type=f32,
                ) * factor
                if index == 0:
                    score = jnp.where(own_visible, score, masked_score)
                score_ref[:, index * rows : (index + 1) * rows] = score
                most = score[:, :HEAD_DIM]
                for start in range(HEAD_DIM, rows, HEAD_DIM):
                    most = jnp.maximum(most, score[:, start : start + HEAD_DIM])
                if index > 0:
                    most = jnp.where(seen[index], most, masked_score)
                highest = jnp.maximum(highest, most)
            highest = jnp.max(highest, axis=-1, keepdims=True)
            totals = jnp.zeros((rows, HEAD_DIM), f32)
            mixed = jnp.zeros((rows, HEAD_DIM), f32)
            for index, keyval_ref in enumerate(keyval_refs):
                ceiling = highest
                if index > 0:
                    ceiling = jnp.where(seen[index], highest, -masked_score)
                expo = jnp.exp2(score_ref[:, index * rows : (index + 1) * rows] - ceiling)
                for start in range(0, rows, HEAD_DIM):
                    totals = totals + expo[:, start : start + HEAD_DIM]
                mixed = mixed + dot(expo.astype(bf16), keyval_ref[:, value_columns])
            total = jnp.sum(totals, axis=-1, keepdims=True)
            context_ref[head] = (mixed / total).astype(bf16)
            return 0

        lax.fori_loop(0, sharing, one_head, 0)

    context = jnp.concatenate([context_ref[head] for head in range(heads)], axis=1)
    step = min(512, send_ref.shape[1])
    for start in range(0, send_ref.shape[1], step):
        columns = slice(start, start + step)
        out = dot(context, weight_ref[:, columns])
        keep_ref[:, columns] = out[:half]
        send_ref[:, columns] = out[half:].astype(bf16)


def placed(choice_ref, plane):
    rows = choice_ref.shape[0]
    first, second = choice_ref[:, 0:1], choice_ref[:, 1:2]
    lane = lax.broadcasted_iota(jnp.int32, (rows, 128), 1)
    goes = jnp.zeros((rows, 128), jnp.bool_)
    for step in range(EXPERTS):
        expert = plane ^ step
        goes = goes | ((lane == step) & ((first == expert) | (second == expert)))
    earlier = (
        lax.broadcasted_iota(jnp.int32, (rows, rows), 1)
        < lax.broadcasted_iota(jnp.int32, (rows, rows), 0)
    )
    slots = dot(earlier.astype(bf16), goes.astype(bf16)).astype(jnp.int32)
    slots = jnp.where(goes, slots, -1)
    return [
        (lane[:, :ROWS] == slots[:, step : step + 1]).astype(bf16) for step in range(EXPERTS)
    ]


def pack_kernel(along, keep_ref, came_ref, tokens_ref, gain_ref, choice_ref, residual_ref, *out_refs):
    attention = keep_ref[...] + came_ref[...].astype(f32)
    residual = (tokens_ref[...].astype(f32) + attention).astype(bf16)
    residual_ref[...] = residual
    mixed_in = normalized(residual.astype(f32), gain_ref[...])
    plane = lax.axis_index("expert") // along
    for out_ref, routing in zip(out_refs, placed(choice_ref, plane)):
        out_ref[...] = lax.dot_general(
            routing, mixed_in, (((0,), (0,)), ((), ())), preferred_element_type=f32
        ).astype(bf16)


def expert_kernel(count, gate_ref, up_ref, down_ref, *refs):
    row_refs, out_refs = refs[:count], refs[count : 2 * count]
    rows_ref, total_ref = refs[2 * count :]
    step = pl.program_id(0)

    @pl.when(step == 0)
    def _():
        for index, row_ref in enumerate(row_refs):
            rows_ref[index * ROWS : (index + 1) * ROWS] = row_ref[...]
        total_ref[...] = jnp.zeros_like(total_ref)

    rows = rows_ref[...]
    gate = dot(rows, gate_ref[...])
    upward = dot(rows, up_ref[...])
    hidden = (gate / (1.0 + jnp.exp(-gate)) * upward).astype(bf16)
    total_ref[...] += dot(hidden, down_ref[...])

    @pl.when(step == pl.num_programs(0) - 1)
    def _():
        for index, out_ref in enumerate(out_refs):
            out_ref[...] = total_ref[index * ROWS : (index + 1) * ROWS].astype(bf16)


def experts(rows, expert_gate, expert_up, expert_down):
    width, hidden = expert_gate.shape
    block = 256
    count = len(rows)
    whole = pl.BlockSpec((ROWS, width), lambda i: (0, 0))
    return pl.pallas_call(
        functools.partial(expert_kernel, count),
        grid=(hidden // block,),
        in_specs=[
            pl.BlockSpec((width, block), lambda i: (0, i)),
            pl.BlockSpec((width, block), lambda i: (0, i)),
            pl.BlockSpec((block, width), lambda i: (i, 0)),
        ]
        + [whole] * count,
        out_specs=[whole] * count,
        out_shape=[jax.ShapeDtypeStruct((ROWS, width), bf16)] * count,
        scratch_shapes=[
            pltpu.VMEM((count * ROWS, width), bf16),
            pltpu.VMEM((count * ROWS, width), f32),
        ],
        compiler_params=pltpu.CompilerParams(vmem_limit_bytes=40 << 20),
        cost_estimate=pl.CostEstimate(
            flops=6 * count * ROWS * width * hidden,
            bytes_accessed=6 * width * hidden,
            transcendentals=0,
        ),
        name="experts",
    )(expert_gate, expert_up, expert_down, *rows)


def combine_kernel(along, residual_ref, choice_ref, weight_ref, *refs):
    row_refs, out_ref = refs[:-1], refs[-1]
    plane = lax.axis_index("expert") // along
    total = residual_ref[...].astype(f32)
    for step, routing in enumerate(placed(choice_ref, plane)):
        expert = plane ^ step
        weight = jnp.sum(
            jnp.where(choice_ref[...] == expert, weight_ref[...], 0.0), axis=1, keepdims=True
        )
        total = total + weight * dot(routing, row_refs[step][...])
    out_ref[...] = total.astype(bf16)


def add(*terms):
    return sum(term.astype(f32) for term in terms).astype(bf16)


def body(
    tokens,
    expert_choice,
    gate_weights,
    attention_gain,
    query_weight,
    key_value_weight,
    output_weight,
    feedforward_gain,
    expert_gate,
    expert_up,
    expert_down,
):
    local_rows, model_width = tokens.shape
    share = query_weight.shape[0]
    cores = lax.axis_size("dp")
    chips = lax.axis_size("expert")
    along = chips // EXPERTS
    query_width = query_weight.shape[1] // cores
    keyval_width = key_value_weight.shape[1] // cores
    heads = query_width // HEAD_DIM
    pair_rows = local_rows * cores
    chip = lax.axis_index("expert")
    core = lax.axis_index("dp")

    def across(x):
        return lax.ppermute(x, "dp", [(i, i ^ 1) for i in range(cores)])

    def beside(x, turn):
        return lax.ppermute(x, "expert", [(i, i ^ turn) for i in range(chips)])

    def upward(x):
        return lax.ppermute(x, "expert", [(i, i + along) for i in range(chips - along)])

    def planes(x, step):
        return lax.ppermute(x, "expert", [(i, i ^ (step * along)) for i in range(chips)])

    order = jnp.arange(pair_rows, dtype=jnp.int32)
    order = (order + core * local_rows) % pair_rows
    positions = chip * pair_rows + order
    halfway = HEAD_DIM // 2
    powers = jnp.arange(halfway, dtype=f32) * (2.0 / HEAD_DIM)
    inverse = base_theta ** (-powers)
    angles = positions.astype(f32)[:, None] * inverse[None, :]
    cosine, sine = jnp.cos(angles), jnp.sin(angles)
    cosine = jnp.concatenate([cosine, cosine], axis=1)
    sine = jnp.concatenate([-sine, sine], axis=1)

    shape = jax.ShapeDtypeStruct
    mine, outgoing = call(
        norm_kernel,
        [shape((local_rows, share), bf16)] * 2,
        (tokens, attention_gain.reshape(1, -1)),
        scratch=[pltpu.VMEM((local_rows, model_width), bf16)],
        flops=8 * local_rows * model_width,
        moved=4 * local_rows * model_width,
        name="norm",
    )
    theirs = across(outgoing)
    keyval_keep, keyval_send = call(
        keyval_kernel,
        [shape((pair_rows, keyval_width), f32)] * 2,
        (mine, theirs, key_value_weight),
        flops=4 * pair_rows * share * keyval_width,
        moved=4 * share * keyval_width,
        name="keyval",
    )
    keyval_came = across(keyval_send)
    query_keep, query_send = call(
        query_kernel,
        [shape((pair_rows, query_width), f32)] * 2,
        (mine, theirs, query_weight),
        flops=4 * pair_rows * share * query_width,
        moved=4 * share * query_width,
        name="query",
    )
    query_came = across(query_send)
    keyval = call(
        keyval_turn_kernel,
        shape((pair_rows, keyval_width), bf16),
        (keyval_keep, keyval_came, cosine, sine),
        flops=8 * pair_rows * keyval_width,
        moved=10 * pair_rows * keyval_width,
        name="keyval_turn",
    )
    queries = call(
        query_turn_kernel,
        shape((heads, pair_rows, HEAD_DIM), bf16),
        (query_keep, query_came, cosine, sine),
        flops=8 * pair_rows * query_width,
        moved=10 * pair_rows * query_width,
        name="query_turn",
    )
    blocks, places = [], []
    line = keyval
    for back in range(EXPERTS):
        if back:
            line = upward(line)
        for turn in range(along):
            blocks.append(beside(line, turn) if turn else line)
            places.append((back, turn))
    attention_send, attention_keep = call(
        functools.partial(attention_kernel, tuple(places), along),
        [shape((local_rows, model_width), bf16), shape((local_rows, model_width), f32)],
        (queries, output_weight, *blocks),
        scratch=[
            pltpu.VMEM((pair_rows, pair_rows * len(blocks)), f32),
            pltpu.VMEM((heads, pair_rows, HEAD_DIM), bf16),
        ],
        flops=4 * pair_rows * pair_rows * len(blocks) * query_width
        + 2 * pair_rows * query_width * model_width,
        moved=2 * query_width * model_width,
        limit=40 << 20,
        name="attention",
    )
    attention_came = across(attention_send)
    residual, *packed = call(
        functools.partial(pack_kernel, along),
        [shape((local_rows, model_width), bf16)] + [shape((ROWS, model_width), bf16)] * EXPERTS,
        (
            attention_keep,
            attention_came,
            tokens,
            feedforward_gain.reshape(1, -1),
            expert_choice,
        ),
        flops=2 * EXPERTS * ROWS * local_rows * model_width,
        moved=12 * local_rows * model_width,
        name="pack",
    )
    collected = []
    for step in range(EXPERTS):
        arrived = planes(packed[step], step) if step else packed[step]
        line = [arrived] + [beside(arrived, turn) for turn in range(1, along)]
        line = line + [across(x) for x in line]
        outs = experts(line, expert_gate, expert_up, expert_down)
        near = [add(own, across(other)) for own, other in zip(outs[:along], outs[along:])]
        reduced = add(near[0], *[beside(near[turn], turn) for turn in range(1, along)])
        collected.append(planes(reduced, step) if step else reduced)
    return call(
        functools.partial(combine_kernel, along),
        shape((local_rows, model_width), bf16),
        (residual, expert_choice, gate_weights, *collected),
        flops=2 * EXPERTS * ROWS * local_rows * model_width,
        moved=8 * local_rows * model_width,
        name="combine",
    )


def solution(mesh):
    assert mesh.shape["dp"] == 2 and mesh.shape["expert"] % EXPERTS == 0
    in_specs = (
        P(("group", "expert", "dp"), None),
        P(("group", "expert", "dp"), None),
        P(("group", "expert", "dp"), None),
        P(),
        P("dp", None),
        P("dp", None),
        P("dp", None),
        P(),
        P(None, ("expert", "dp")),
        P(None, ("expert", "dp")),
        P(("expert", "dp"), None),
    )
    out_specs = P(("group", "expert", "dp"), None)
    return jax.shard_map(body, mesh=mesh, in_specs=in_specs, out_specs=out_specs, check_vma=False)
```

```python
import functools
import math

import jax
import jax.numpy as jnp
from jax import lax
from jax.experimental import pallas as pl
from jax.experimental.pallas import tpu as pltpu
from jax.sharding import PartitionSpec as P


HEAD_DIM = 128
EXPERTS = 4
CAP = 70
ROWS = -(-CAP // 8) * 8

HIDDEN_STEP = 256
DOWN_STEP = 256
ORDER = (0, 1, 2, 3)

epsilon = 1e-05
base_theta = 1000000.0
masked_score = -1e30

VMEM = pl.BlockSpec(memory_space=pltpu.VMEM)
f32 = jnp.float32
bf16 = jnp.bfloat16


def dot(a, b):
    return jnp.dot(a, b, preferred_element_type=f32)


def call(kernel, outs, operands, scratch=(), flops=0, moved=0, limit=16 << 20):
    return pl.pallas_call(
        kernel,
        out_shape=outs,
        in_specs=[VMEM] * len(operands),
        out_specs=jax.tree.map(lambda _: VMEM, outs),
        scratch_shapes=list(scratch),
        compiler_params=pltpu.CompilerParams(vmem_limit_bytes=limit),
        cost_estimate=pl.CostEstimate(flops=flops, bytes_accessed=moved, transcendentals=0),
    )(*operands)


def normalized(widened, gain):
    spread = jnp.mean(widened * widened, axis=-1, keepdims=True)
    return (widened * lax.rsqrt(spread + epsilon) * gain).astype(bf16)


def norm_kernel(tokens_ref, gain_ref, keep_ref, send_ref, whole_ref):
    half = keep_ref.shape[1]
    whole_ref[...] = normalized(tokens_ref[...].astype(f32), gain_ref[...])
    core = lax.axis_index("dp")
    keep_ref[...] = whole_ref[:, pl.ds(pl.multiple_of(core * half, half), half)]
    send_ref[...] = whole_ref[:, pl.ds(pl.multiple_of((1 - core) * half, half), half)]


def keyval_kernel(mine_ref, theirs_ref, weight_ref, keep_ref, send_ref):
    rows = jnp.concatenate([mine_ref[...], theirs_ref[...]], axis=0)
    width = keep_ref.shape[1] // 2
    core = lax.axis_index("dp")
    for out_ref, owner in ((send_ref, 1 - core), (keep_ref, core)):
        for part in range(2):
            start = pl.multiple_of((part * 2 + owner) * width, width)
            out_ref[:, part * width : (part + 1) * width] = dot(
                rows, weight_ref[:, pl.ds(start, width)]
            )


def query_kernel(mine_ref, theirs_ref, weight_ref, keep_ref, send_ref):
    rows = jnp.concatenate([mine_ref[...], theirs_ref[...]], axis=0)
    width = keep_ref.shape[1]
    step = min(512, width)
    core = lax.axis_index("dp")
    for out_ref, owner in ((send_ref, 1 - core), (keep_ref, core)):
        for offset in range(0, width, step):
            start = pl.multiple_of(owner * width + offset, step)
            out_ref[:, offset : offset + step] = dot(rows, weight_ref[:, pl.ds(start, step)])


def summed(keep_ref, came_ref, columns):
    half = keep_ref.shape[0] // 2
    came = came_ref[:, columns]
    return keep_ref[:, columns] + jnp.concatenate([came[half:], came[:half]], axis=0)


def turned(vectors, cosine, sine):
    return vectors * cosine + pltpu.roll(vectors, HEAD_DIM // 2, 1) * sine


def keyval_turn_kernel(keep_ref, came_ref, cosine_ref, sine_ref, out_ref):
    width = out_ref.shape[1]
    for start in range(0, width, HEAD_DIM):
        columns = slice(start, start + HEAD_DIM)
        total = summed(keep_ref, came_ref, columns)
        if start < width // 2:
            total = turned(total, cosine_ref[...], sine_ref[...])
        out_ref[:, columns] = total.astype(bf16)


def query_turn_kernel(keep_ref, came_ref, cosine_ref, sine_ref, out_ref):
    for head in range(out_ref.shape[0]):
        columns = slice(head * HEAD_DIM, (head + 1) * HEAD_DIM)
        total = summed(keep_ref, came_ref, columns)
        out_ref[head] = turned(total, cosine_ref[...], sine_ref[...]).astype(bf16)


def attention_kernel(places, along, query_ref, weight_ref, *refs):
    keyval_refs = refs[: len(places)]
    send_ref, keep_ref, score_ref, context_ref = refs[len(places) :]
    heads, rows, _ = query_ref.shape
    half = rows // 2
    shared = keyval_refs[0].shape[1] // (2 * HEAD_DIM)
    sharing = heads // shared
    core = lax.axis_index("dp")
    chip = lax.axis_index("expert")
    plane, place = chip // along, chip % along

    def position(shape, axis):
        row = lax.broadcasted_iota(jnp.int32, shape, axis)
        return jnp.where(core == 0, row, jnp.where(row < half, row + half, row - half))

    own_visible = position((rows, rows), 1) <= position((rows, rows), 0)
    seen = []
    for back, turn in places:
        if back == 0:
            seen.append((place ^ turn) < place)
        else:
            seen.append(plane >= back)
    factor = HEAD_DIM ** (-0.5) * math.log2(math.e)

    for group in range(shared):
        key_columns = slice(group * HEAD_DIM, (group + 1) * HEAD_DIM)
        value_columns = slice((shared + group) * HEAD_DIM, (shared + group + 1) * HEAD_DIM)

        def one_head(member, _):
            head = group * sharing + member
            query = query_ref[head]
            highest = jnp.full((rows, HEAD_DIM), masked_score, f32)
            for index, keyval_ref in enumerate(keyval_refs):
                score = lax.dot_general(
                    query,
                    keyval_ref[:, key_columns],
                    (((1,), (1,)), ((), ())),
                    preferred_element_type=f32,
                ) * factor
                if index == 0:
                    score = jnp.where(own_visible, score, masked_score)
                score_ref[:, index * rows : (index + 1) * rows] = score
                most = score[:, :HEAD_DIM]
                for start in range(HEAD_DIM, rows, HEAD_DIM):
                    most = jnp.maximum(most, score[:, start : start + HEAD_DIM])
                if index > 0:
                    most = jnp.where(seen[index], most, masked_score)
                highest = jnp.maximum(highest, most)
            highest = jnp.max(highest, axis=-1, keepdims=True)
            totals = jnp.zeros((rows, HEAD_DIM), f32)
            mixed = jnp.zeros((rows, HEAD_DIM), f32)
            for index, keyval_ref in enumerate(keyval_refs):
                ceiling = highest
                if index > 0:
                    ceiling = jnp.where(seen[index], highest, -masked_score)
                expo = jnp.exp2(score_ref[:, index * rows : (index + 1) * rows] - ceiling)
                for start in range(0, rows, HEAD_DIM):
                    totals = totals + expo[:, start : start + HEAD_DIM]
                mixed = mixed + dot(expo.astype(bf16), keyval_ref[:, value_columns])
            total = jnp.sum(totals, axis=-1, keepdims=True)
            context_ref[head] = (mixed / total).astype(bf16)
            return 0

        lax.fori_loop(0, sharing, one_head, 0)

    context = jnp.concatenate([context_ref[head] for head in range(heads)], axis=1)
    step = min(512, send_ref.shape[1])
    for start in range(0, send_ref.shape[1], step):
        columns = slice(start, start + step)
        out = dot(context, weight_ref[:, columns])
        keep_ref[:, columns] = out[:half]
        send_ref[:, columns] = out[half:].astype(bf16)


def as_columns(rows_ref):
    count = rows_ref.shape[1]
    same = (
        lax.broadcasted_iota(jnp.int32, (count, count), 0)
        == lax.broadcasted_iota(jnp.int32, (count, count), 1)
    )
    return lax.dot_general(
        same.astype(f32),
        rows_ref[...].astype(f32),
        (((1,), (1,)), ((), ())),
        precision=lax.Precision.HIGHEST,
        preferred_element_type=f32,
    )


def placed(choice, plane):
    rows = choice.shape[0]
    first, second = choice[:, 0:1], choice[:, 1:2]
    lane = lax.broadcasted_iota(jnp.int32, (rows, 128), 1)
    goes = jnp.zeros((rows, 128), jnp.bool_)
    for step in range(EXPERTS):
        expert = plane ^ step
        goes = goes | ((lane == step) & ((first == expert) | (second == expert)))
    earlier = (
        lax.broadcasted_iota(jnp.int32, (rows, rows), 1)
        < lax.broadcasted_iota(jnp.int32, (rows, rows), 0)
    )
    slots = dot(earlier.astype(bf16), goes.astype(bf16)).astype(jnp.int32)
    slots = jnp.where(goes, slots, -1)
    return [
        (lane[:, :ROWS] == slots[:, step : step + 1]).astype(bf16) for step in range(EXPERTS)
    ]


def pack_kernel(along, keep_ref, came_ref, tokens_ref, gain_ref, choice_ref, residual_ref, *out_refs):
    attention = keep_ref[...] + came_ref[...].astype(f32)
    residual = (tokens_ref[...].astype(f32) + attention).astype(bf16)
    residual_ref[...] = residual
    mixed_in = normalized(residual.astype(f32), gain_ref[...])
    plane = lax.axis_index("expert") // along
    choice = as_columns(choice_ref).astype(jnp.int32)
    for out_ref, routing in zip(out_refs, placed(choice, plane)):
        out_ref[...] = lax.dot_general(
            routing, mixed_in, (((0,), (0,)), ((), ())), preferred_element_type=f32
        ).astype(bf16)


def fetch_kernel(parts, from_ref, to_ref, sem):
    rows = from_ref.shape[0] // parts
    copies = []
    for part in range(parts):
        block = pl.ds(part * rows, rows)
        copies.append(
            pltpu.make_async_copy(from_ref.at[block], to_ref.at[block], sem.at[part])
        )
    for copy in copies:
        copy.start()
    for copy in copies:
        copy.wait()


def fetched(weight):
    parts = 4
    return pl.pallas_call(
        functools.partial(fetch_kernel, parts),
        out_shape=jax.ShapeDtypeStruct(weight.shape, weight.dtype),
        in_specs=[pl.BlockSpec(memory_space=pltpu.HBM)],
        out_specs=VMEM,
        scratch_shapes=[pltpu.SemaphoreType.DMA((parts,))],
        compiler_params=pltpu.CompilerParams(vmem_limit_bytes=2 << 20),
        cost_estimate=pl.CostEstimate(
            flops=0, bytes_accessed=4 * weight.size, transcendentals=0
        ),
        name="fetch",
    )(weight)


def expert_kernel(count, gate_ref, up_ref, down_ref, *refs):
    row_refs, out_refs, hidden_ref = refs[:count], refs[count : 2 * count], refs[2 * count]
    rows = jnp.concatenate([row_ref[...] for row_ref in row_refs], axis=0)
    for start in range(0, hidden_ref.shape[1], HIDDEN_STEP):
        columns = slice(start, start + HIDDEN_STEP)
        gate = dot(rows, gate_ref[:, columns])
        upward = dot(rows, up_ref[:, columns])
        hidden_ref[:, columns] = (gate / (1.0 + jnp.exp(-gate)) * upward).astype(bf16)
    hidden = hidden_ref[...]
    for start in range(0, down_ref.shape[1], DOWN_STEP):
        columns = slice(start, start + DOWN_STEP)
        out = dot(hidden, down_ref[:, columns]).astype(bf16)
        for index, out_ref in enumerate(out_refs):
            out_ref[:, columns] = out[index * ROWS : (index + 1) * ROWS]


def experts(rows, expert_gate, expert_up, expert_down):
    width, hidden = expert_gate.shape
    count = len(rows)
    return call(
        functools.partial(expert_kernel, count),
        [jax.ShapeDtypeStruct((ROWS, width), bf16)] * count,
        (expert_gate, expert_up, expert_down, *rows),
        scratch=[pltpu.VMEM((count * ROWS, hidden), bf16)],
        flops=6 * count * ROWS * width * hidden,
        moved=6 * width * hidden,
        limit=12 << 20,
    )


def combine_kernel(along, residual_ref, choice_ref, weight_ref, *refs):
    row_refs, out_ref = refs[:-1], refs[-1]
    plane = lax.axis_index("expert") // along
    choice = as_columns(choice_ref).astype(jnp.int32)
    weights = as_columns(weight_ref)
    total = residual_ref[...].astype(f32)
    for step, routing in enumerate(placed(choice, plane)):
        expert = plane ^ step
        weight = jnp.sum(jnp.where(choice == expert, weights, 0.0), axis=1, keepdims=True)
        total = total + weight * dot(routing, row_refs[step][...])
    out_ref[...] = total.astype(bf16)


def add(*terms):
    return sum(term.astype(f32) for term in terms).astype(bf16)


def body(
    tokens,
    expert_choice,
    gate_weights,
    attention_gain,
    query_weight,
    key_value_weight,
    output_weight,
    feedforward_gain,
    expert_gate,
    expert_up,
    expert_down,
):
    local_rows, model_width = tokens.shape
    share = query_weight.shape[0]
    cores = lax.axis_size("dp")
    chips = lax.axis_size("expert")
    along = chips // EXPERTS
    query_width = query_weight.shape[1] // cores
    keyval_width = key_value_weight.shape[1] // cores
    heads = query_width // HEAD_DIM
    pair_rows = local_rows * cores
    chip = lax.axis_index("expert")
    core = lax.axis_index("dp")

    def across(x):
        return lax.ppermute(x, "dp", [(i, i ^ 1) for i in range(cores)])

    def beside(x, turn):
        return lax.ppermute(x, "expert", [(i, i ^ turn) for i in range(chips)])

    def upward(x):
        return lax.ppermute(x, "expert", [(i, (i + along) % chips) for i in range(chips)])

    def planes(x, step):
        return lax.ppermute(x, "expert", [(i, i ^ (step * along)) for i in range(chips)])

    order = jnp.arange(pair_rows, dtype=jnp.int32)
    order = (order + core * local_rows) % pair_rows
    positions = chip * pair_rows + order
    halfway = HEAD_DIM // 2
    powers = jnp.arange(halfway, dtype=f32) * (2.0 / HEAD_DIM)
    inverse = base_theta ** (-powers)
    angles = positions.astype(f32)[:, None] * inverse[None, :]
    cosine, sine = jnp.cos(angles), jnp.sin(angles)
    cosine = jnp.concatenate([cosine, cosine], axis=1)
    sine = jnp.concatenate([-sine, sine], axis=1)

    shape = jax.ShapeDtypeStruct
    mine, outgoing = call(
        norm_kernel,
        [shape((local_rows, share), bf16)] * 2,
        (tokens, attention_gain.reshape(1, -1)),
        scratch=[pltpu.VMEM((local_rows, model_width), bf16)],
        flops=8 * local_rows * model_width,
        moved=4 * local_rows * model_width,
    )
    theirs = across(outgoing)
    keyval_keep, keyval_send = call(
        keyval_kernel,
        [shape((pair_rows, keyval_width), f32)] * 2,
        (mine, theirs, key_value_weight),
        flops=4 * pair_rows * share * keyval_width,
        moved=4 * share * keyval_width,
    )
    keyval_came = across(keyval_send)
    query_keep, query_send = call(
        query_kernel,
        [shape((pair_rows, query_width), f32)] * 2,
        (mine, theirs, query_weight),
        flops=4 * pair_rows * share * query_width,
        moved=4 * share * query_width,
    )
    query_came = across(query_send)
    keyval = call(
        keyval_turn_kernel,
        shape((pair_rows, keyval_width), bf16),
        (keyval_keep, keyval_came, cosine, sine),
        flops=8 * pair_rows * keyval_width,
        moved=10 * pair_rows * keyval_width,
    )
    queries = call(
        query_turn_kernel,
        shape((heads, pair_rows, HEAD_DIM), bf16),
        (query_keep, query_came, cosine, sine),
        flops=8 * pair_rows * query_width,
        moved=10 * pair_rows * query_width,
    )
    blocks, places = [], []
    line = keyval
    for back in range(EXPERTS):
        if back:
            line = upward(line)
        for turn in range(along):
            blocks.append(beside(line, turn) if turn else line)
            places.append((back, turn))
    attention_send, attention_keep = call(
        functools.partial(attention_kernel, tuple(places), along),
        [shape((local_rows, model_width), bf16), shape((local_rows, model_width), f32)],
        (queries, output_weight, *blocks),
        scratch=[
            pltpu.VMEM((pair_rows, pair_rows * len(blocks)), f32),
            pltpu.VMEM((heads, pair_rows, HEAD_DIM), bf16),
        ],
        flops=4 * pair_rows * pair_rows * len(blocks) * query_width
        + 2 * pair_rows * query_width * model_width,
        moved=2 * query_width * model_width,
        limit=20 << 20,
    )
    attention_came = across(attention_send)
    residual, *packed = call(
        functools.partial(pack_kernel, along),
        [shape((local_rows, model_width), bf16)] + [shape((ROWS, model_width), bf16)] * EXPERTS,
        (
            attention_keep,
            attention_came,
            tokens,
            feedforward_gain.reshape(1, -1),
            expert_choice.T,
        ),
        flops=2 * EXPERTS * ROWS * local_rows * model_width,
        moved=12 * local_rows * model_width,
    )
    expert_gate = fetched(expert_gate)
    expert_up = fetched(expert_up)
    expert_down = fetched(expert_down)
    arrived = {}
    for step in ORDER:
        arrived[step] = planes(packed[step], step) if step else packed[step]
    collected = [None] * EXPERTS
    for step in ORDER:
        line = [arrived[step]] + [beside(arrived[step], turn) for turn in range(1, along)]
        line = line + [across(x) for x in line]
        outs = experts(line, expert_gate, expert_up, expert_down)
        others = [across(x) for x in outs[along:]]
        near = [add(own, other) for own, other in zip(outs[:along], others)]
        others = [beside(near[turn], turn) for turn in range(1, along)]
        reduced = add(near[0], *others)
        collected[step] = planes(reduced, step) if step else reduced
    return call(
        functools.partial(combine_kernel, along),
        shape((local_rows, model_width), bf16),
        (residual, expert_choice.T, gate_weights.T, *collected),
        flops=2 * EXPERTS * ROWS * local_rows * model_width,
        moved=8 * local_rows * model_width,
    )


def solution(mesh):
    assert mesh.shape["dp"] == 2 and mesh.shape["expert"] % EXPERTS == 0
    in_specs = (
        P(("group", "expert", "dp"), None),
        P(("group", "expert", "dp"), None),
        P(("group", "expert", "dp"), None),
        P(),
        P("dp", None),
        P("dp", None),
        P("dp", None),
        P(),
        P(None, ("expert", "dp")),
        P(None, ("expert", "dp")),
        P(("expert", "dp"), None),
    )
    out_specs = P(("group", "expert", "dp"), None)

    return jax.shard_map(body, mesh=mesh, in_specs=in_specs, out_specs=out_specs, check_vma=False)
```

```python
import functools
import math

import jax
import jax.numpy as jnp
from jax import lax
from jax.experimental import pallas as pl
from jax.experimental.pallas import tpu as pltpu
from jax.sharding import PartitionSpec as P


HEAD_DIM = 128
EXPERTS = 4
CAP = 70
ROWS = -(-CAP // 8) * 8

HIDDEN_STEP = 256
DOWN_STEP = 256
ORDER = (0, 2, 1, 3)

epsilon = 1e-05
base_theta = 1000000.0
masked_score = -1e30

VMEM = pl.BlockSpec(memory_space=pltpu.VMEM)
f32 = jnp.float32
bf16 = jnp.bfloat16


def dot(a, b):
    return jnp.dot(a, b, preferred_element_type=f32)


def call(kernel, outs, operands, scratch=(), flops=0, moved=0, limit=16 << 20):
    return pl.pallas_call(
        kernel,
        out_shape=outs,
        in_specs=[VMEM] * len(operands),
        out_specs=jax.tree.map(lambda _: VMEM, outs),
        scratch_shapes=list(scratch),
        compiler_params=pltpu.CompilerParams(vmem_limit_bytes=limit),
        cost_estimate=pl.CostEstimate(flops=flops, bytes_accessed=moved, transcendentals=0),
    )(*operands)


def normalized(widened, gain):
    spread = jnp.mean(widened * widened, axis=-1, keepdims=True)
    return (widened * lax.rsqrt(spread + epsilon) * gain).astype(bf16)


def norm_kernel(tokens_ref, gain_ref, keep_ref, send_ref, whole_ref):
    half = keep_ref.shape[1]
    whole_ref[...] = normalized(tokens_ref[...].astype(f32), gain_ref[...])
    core = lax.axis_index("dp")
    keep_ref[...] = whole_ref[:, pl.ds(pl.multiple_of(core * half, half), half)]
    send_ref[...] = whole_ref[:, pl.ds(pl.multiple_of((1 - core) * half, half), half)]


def keyval_kernel(mine_ref, theirs_ref, weight_ref, keep_ref, send_ref):
    rows = jnp.concatenate([mine_ref[...], theirs_ref[...]], axis=0)
    width = keep_ref.shape[1] // 2
    core = lax.axis_index("dp")
    for out_ref, owner in ((send_ref, 1 - core), (keep_ref, core)):
        for part in range(2):
            start = pl.multiple_of((part * 2 + owner) * width, width)
            out_ref[:, part * width : (part + 1) * width] = dot(
                rows, weight_ref[:, pl.ds(start, width)]
            )


def query_kernel(mine_ref, theirs_ref, weight_ref, keep_ref, send_ref):
    rows = jnp.concatenate([mine_ref[...], theirs_ref[...]], axis=0)
    width = keep_ref.shape[1]
    step = min(512, width)
    core = lax.axis_index("dp")
    for out_ref, owner in ((send_ref, 1 - core), (keep_ref, core)):
        for offset in range(0, width, step):
            start = pl.multiple_of(owner * width + offset, step)
            out_ref[:, offset : offset + step] = dot(rows, weight_ref[:, pl.ds(start, step)])


def summed(keep_ref, came_ref, columns):
    half = keep_ref.shape[0] // 2
    came = came_ref[:, columns]
    return keep_ref[:, columns] + jnp.concatenate([came[half:], came[:half]], axis=0)


def turned(vectors, cosine, sine):
    return vectors * cosine + pltpu.roll(vectors, HEAD_DIM // 2, 1) * sine


def keyval_turn_kernel(keep_ref, came_ref, cosine_ref, sine_ref, out_ref):
    width = out_ref.shape[1]
    for start in range(0, width, HEAD_DIM):
        columns = slice(start, start + HEAD_DIM)
        total = summed(keep_ref, came_ref, columns)
        if start < width // 2:
            total = turned(total, cosine_ref[...], sine_ref[...])
        out_ref[:, columns] = total.astype(bf16)


def query_turn_kernel(keep_ref, came_ref, cosine_ref, sine_ref, out_ref):
    for head in range(out_ref.shape[0]):
        columns = slice(head * HEAD_DIM, (head + 1) * HEAD_DIM)
        total = summed(keep_ref, came_ref, columns)
        out_ref[head] = turned(total, cosine_ref[...], sine_ref[...]).astype(bf16)


def attention_kernel(places, along, first, last, query_ref, *refs):
    refs = list(refs)
    keyval_refs = [refs.pop(0) for _ in places]
    before = [] if first else [refs.pop(0) for _ in range(3)]
    weight_ref = refs.pop(0) if last else None
    after = [refs.pop(0) for _ in range(2 if last else 3)]
    score_ref = refs.pop(0)
    context_ref = refs.pop(0) if last else None
    heads, rows, _ = query_ref.shape
    half = rows // 2
    shared = keyval_refs[0].shape[1] // (2 * HEAD_DIM)
    sharing = heads // shared
    core = lax.axis_index("dp")
    chip = lax.axis_index("expert")
    plane, place = chip // along, chip % along

    def position(shape, axis):
        row = lax.broadcasted_iota(jnp.int32, shape, axis)
        return jnp.where(core == 0, row, jnp.where(row < half, row + half, row - half))

    if first:
        own_visible = position((rows, rows), 1) <= position((rows, rows), 0)
    seen = []
    for back, turn in places:
        if back == 0:
            seen.append((place ^ turn) < place)
        else:
            seen.append(plane >= back)
    factor = HEAD_DIM ** (-0.5) * math.log2(math.e)

    for group in range(shared):
        key_columns = slice(group * HEAD_DIM, (group + 1) * HEAD_DIM)
        value_columns = slice((shared + group) * HEAD_DIM, (shared + group + 1) * HEAD_DIM)

        def one_head(member, _):
            head = group * sharing + member
            query = query_ref[head]
            highest = jnp.full((rows, HEAD_DIM), masked_score, f32)
            for index, keyval_ref in enumerate(keyval_refs):
                score = lax.dot_general(
                    query,
                    keyval_ref[:, key_columns],
                    (((1,), (1,)), ((), ())),
                    preferred_element_type=f32,
                ) * factor
                own = first and index == 0
                if own:
                    score = jnp.where(own_visible, score, masked_score)
                score_ref[:, index * rows : (index + 1) * rows] = score
                most = score[:, :HEAD_DIM]
                for start in range(HEAD_DIM, rows, HEAD_DIM):
                    most = jnp.maximum(most, score[:, start : start + HEAD_DIM])
                if not own:
                    most = jnp.where(seen[index], most, masked_score)
                highest = jnp.maximum(highest, most)
            highest = jnp.max(highest, axis=-1, keepdims=True)
            if first:
                totals = jnp.zeros((rows, HEAD_DIM), f32)
                mixed = jnp.zeros((rows, HEAD_DIM), f32)
            else:
                earlier = before[0][head][:, :1]
                highest = jnp.maximum(highest, earlier)
                shrink = jnp.exp2(earlier - highest)
                totals = before[1][head] * shrink
                mixed = before[2][head] * shrink
            for index, keyval_ref in enumerate(keyval_refs):
                ceiling = highest
                if not (first and index == 0):
                    ceiling = jnp.where(seen[index], highest, -masked_score)
                expo = jnp.exp2(score_ref[:, index * rows : (index + 1) * rows] - ceiling)
                for start in range(0, rows, HEAD_DIM):
                    totals = totals + expo[:, start : start + HEAD_DIM]
                mixed = mixed + dot(expo.astype(bf16), keyval_ref[:, value_columns])
            if last:
                total = jnp.sum(totals, axis=-1, keepdims=True)
                context_ref[head] = (mixed / total).astype(bf16)
            else:
                after[0][head] = jnp.broadcast_to(highest, (rows, HEAD_DIM))
                after[1][head] = totals
                after[2][head] = mixed
            return 0

        lax.fori_loop(0, sharing, one_head, 0)

    if last:
        send_ref, keep_ref = after
        context = jnp.concatenate([context_ref[head] for head in range(heads)], axis=1)
        step = min(512, send_ref.shape[1])
        for start in range(0, send_ref.shape[1], step):
            columns = slice(start, start + step)
            out = dot(context, weight_ref[:, columns])
            keep_ref[:, columns] = out[:half]
            send_ref[:, columns] = out[half:].astype(bf16)


def as_columns(rows_ref):
    count = rows_ref.shape[1]
    same = (
        lax.broadcasted_iota(jnp.int32, (count, count), 0)
        == lax.broadcasted_iota(jnp.int32, (count, count), 1)
    )
    return lax.dot_general(
        same.astype(f32),
        rows_ref[...].astype(f32),
        (((1,), (1,)), ((), ())),
        precision=lax.Precision.HIGHEST,
        preferred_element_type=f32,
    )


def placed(choice, plane):
    rows = choice.shape[0]
    first, second = choice[:, 0:1], choice[:, 1:2]
    lane = lax.broadcasted_iota(jnp.int32, (rows, 128), 1)
    goes = jnp.zeros((rows, 128), jnp.bool_)
    for step in range(EXPERTS):
        expert = plane ^ step
        goes = goes | ((lane == step) & ((first == expert) | (second == expert)))
    earlier = (
        lax.broadcasted_iota(jnp.int32, (rows, rows), 1)
        < lax.broadcasted_iota(jnp.int32, (rows, rows), 0)
    )
    slots = dot(earlier.astype(bf16), goes.astype(bf16)).astype(jnp.int32)
    slots = jnp.where(goes, slots, -1)
    return [
        (lane[:, :ROWS] == slots[:, step : step + 1]).astype(bf16) for step in range(EXPERTS)
    ]


def pack_kernel(along, keep_ref, came_ref, tokens_ref, gain_ref, choice_ref, residual_ref, *out_refs):
    attention = keep_ref[...] + came_ref[...].astype(f32)
    residual = (tokens_ref[...].astype(f32) + attention).astype(bf16)
    residual_ref[...] = residual
    mixed_in = normalized(residual.astype(f32), gain_ref[...])
    plane = lax.axis_index("expert") // along
    choice = as_columns(choice_ref).astype(jnp.int32)
    for out_ref, routing in zip(out_refs, placed(choice, plane)):
        out_ref[...] = lax.dot_general(
            routing, mixed_in, (((0,), (0,)), ((), ())), preferred_element_type=f32
        ).astype(bf16)


def fetch_kernel(parts, from_ref, to_ref, sem):
    rows = from_ref.shape[0] // parts
    copies = []
    for part in range(parts):
        block = pl.ds(part * rows, rows)
        copies.append(
            pltpu.make_async_copy(from_ref.at[block], to_ref.at[block], sem.at[part])
        )
    for copy in copies:
        copy.start()
    for copy in copies:
        copy.wait()


def fetched(weight):
    parts = 4
    return pl.pallas_call(
        functools.partial(fetch_kernel, parts),
        out_shape=jax.ShapeDtypeStruct(weight.shape, weight.dtype),
        in_specs=[pl.BlockSpec(memory_space=pltpu.HBM)],
        out_specs=VMEM,
        scratch_shapes=[pltpu.SemaphoreType.DMA((parts,))],
        compiler_params=pltpu.CompilerParams(vmem_limit_bytes=2 << 20),
        cost_estimate=pl.CostEstimate(
            flops=0, bytes_accessed=4 * weight.size, transcendentals=0
        ),
        name="fetch",
    )(weight)


def expert_kernel(count, gate_ref, up_ref, down_ref, *refs):
    row_refs, out_refs, hidden_ref = refs[:count], refs[count : 2 * count], refs[2 * count]
    rows = jnp.concatenate([row_ref[...] for row_ref in row_refs], axis=0)
    for start in range(0, hidden_ref.shape[1], HIDDEN_STEP):
        columns = slice(start, start + HIDDEN_STEP)
        gate = dot(rows, gate_ref[:, columns])
        upward = dot(rows, up_ref[:, columns])
        hidden_ref[:, columns] = (gate / (1.0 + jnp.exp(-gate)) * upward).astype(bf16)
    hidden = hidden_ref[...]
    for start in range(0, down_ref.shape[1], DOWN_STEP):
        columns = slice(start, start + DOWN_STEP)
        out = dot(hidden, down_ref[:, columns]).astype(bf16)
        for index, out_ref in enumerate(out_refs):
            out_ref[:, columns] = out[index * ROWS : (index + 1) * ROWS]


def experts(rows, expert_gate, expert_up, expert_down):
    width, hidden = expert_gate.shape
    count = len(rows)
    return call(
        functools.partial(expert_kernel, count),
        [jax.ShapeDtypeStruct((ROWS, width), bf16)] * count,
        (expert_gate, expert_up, expert_down, *rows),
        scratch=[pltpu.VMEM((count * ROWS, hidden), bf16)],
        flops=6 * count * ROWS * width * hidden,
        moved=6 * width * hidden,
        limit=12 << 20,
    )


def combine_kernel(along, steps, base_ref, choice_ref, weight_ref, *refs):
    row_refs, out_ref = refs[:-1], refs[-1]
    plane = lax.axis_index("expert") // along
    choice = as_columns(choice_ref).astype(jnp.int32)
    weights = as_columns(weight_ref)
    total = base_ref[...].astype(f32)
    routings = placed(choice, plane)
    for step, row_ref in zip(steps, row_refs):
        expert = plane ^ step
        weight = jnp.sum(jnp.where(choice == expert, weights, 0.0), axis=1, keepdims=True)
        total = total + weight * dot(routings[step], row_ref[...])
    out_ref[...] = total.astype(out_ref.dtype)


def add(*terms):
    return sum(term.astype(f32) for term in terms).astype(bf16)


def body(
    tokens,
    expert_choice,
    gate_weights,
    attention_gain,
    query_weight,
    key_value_weight,
    output_weight,
    feedforward_gain,
    expert_gate,
    expert_up,
    expert_down,
):
    local_rows, model_width = tokens.shape
    share = query_weight.shape[0]
    cores = lax.axis_size("dp")
    chips = lax.axis_size("expert")
    along = chips // EXPERTS
    query_width = query_weight.shape[1] // cores
    keyval_width = key_value_weight.shape[1] // cores
    heads = query_width // HEAD_DIM
    pair_rows = local_rows * cores
    chip = lax.axis_index("expert")
    core = lax.axis_index("dp")

    def across(x):
        return lax.ppermute(x, "dp", [(i, i ^ 1) for i in range(cores)])

    def beside(x, turn):
        return lax.ppermute(x, "expert", [(i, i ^ turn) for i in range(chips)])

    def upward(x):
        return lax.ppermute(x, "expert", [(i, (i + along) % chips) for i in range(chips)])

    def planes(x, step):
        return lax.ppermute(x, "expert", [(i, i ^ (step * along)) for i in range(chips)])

    order = jnp.arange(pair_rows, dtype=jnp.int32)
    order = (order + core * local_rows) % pair_rows
    positions = chip * pair_rows + order
    halfway = HEAD_DIM // 2
    powers = jnp.arange(halfway, dtype=f32) * (2.0 / HEAD_DIM)
    inverse = base_theta ** (-powers)
    angles = positions.astype(f32)[:, None] * inverse[None, :]
    cosine, sine = jnp.cos(angles), jnp.sin(angles)
    cosine = jnp.concatenate([cosine, cosine], axis=1)
    sine = jnp.concatenate([-sine, sine], axis=1)

    shape = jax.ShapeDtypeStruct
    mine, outgoing = call(
        norm_kernel,
        [shape((local_rows, share), bf16)] * 2,
        (tokens, attention_gain.reshape(1, -1)),
        scratch=[pltpu.VMEM((local_rows, model_width), bf16)],
        flops=8 * local_rows * model_width,
        moved=4 * local_rows * model_width,
    )
    theirs = across(outgoing)
    key_value_weight = fetched(key_value_weight)
    keyval_keep, keyval_send = call(
        keyval_kernel,
        [shape((pair_rows, keyval_width), f32)] * 2,
        (mine, theirs, key_value_weight),
        flops=4 * pair_rows * share * keyval_width,
        moved=4 * share * keyval_width,
    )
    keyval_came = across(keyval_send)
    query_keep, query_send = call(
        query_kernel,
        [shape((pair_rows, query_width), f32)] * 2,
        (mine, theirs, query_weight),
        flops=4 * pair_rows * share * query_width,
        moved=4 * share * query_width,
    )
    query_came = across(query_send)
    keyval = call(
        keyval_turn_kernel,
        shape((pair_rows, keyval_width), bf16),
        (keyval_keep, keyval_came, cosine, sine),
        flops=8 * pair_rows * keyval_width,
        moved=10 * pair_rows * keyval_width,
    )
    queries = call(
        query_turn_kernel,
        shape((heads, pair_rows, HEAD_DIM), bf16),
        (query_keep, query_came, cosine, sine),
        flops=8 * pair_rows * query_width,
        moved=10 * pair_rows * query_width,
    )
    parts, part = [], []
    line = keyval
    for back in range(EXPERTS):
        if back:
            line = upward(line)
        part.append((line, (back, 0)))
        if back:
            parts.append(part)
            part = []
        part += [(beside(line, turn), (back, turn)) for turn in range(1, along)]
    parts.append(part)
    state = []
    for index, part in enumerate(parts):
        blocks, places = zip(*part) if part else ((), ())
        last = index == len(parts) - 1
        outs = [shape((heads, pair_rows, HEAD_DIM), f32)] * 3
        scratch = [pltpu.VMEM((pair_rows, pair_rows * max(1, len(blocks))), f32)]
        if last:
            outs = [shape((local_rows, model_width), bf16), shape((local_rows, model_width), f32)]
            scratch.append(pltpu.VMEM((heads, pair_rows, HEAD_DIM), bf16))
        state = call(
            functools.partial(attention_kernel, places, along, index == 0, last),
            outs,
            (queries, *blocks, *state, *([output_weight] if last else [])),
            scratch=scratch,
            flops=4 * pair_rows * pair_rows * len(blocks) * query_width
            + 2 * pair_rows * query_width * model_width * last,
            moved=8 * pair_rows * query_width,
            limit=8 << 20,
        )
    attention_send, attention_keep = state
    attention_came = across(attention_send)
    residual, *packed = call(
        functools.partial(pack_kernel, along),
        [shape((local_rows, model_width), bf16)] + [shape((ROWS, model_width), bf16)] * EXPERTS,
        (
            attention_keep,
            attention_came,
            tokens,
            feedforward_gain.reshape(1, -1),
            expert_choice.T,
        ),
        flops=2 * EXPERTS * ROWS * local_rows * model_width,
        moved=12 * local_rows * model_width,
    )
    expert_gate = fetched(expert_gate)
    expert_up = fetched(expert_up)
    expert_down = fetched(expert_down)
    arrived = {}
    for step in ORDER:
        arrived[step] = planes(packed[step], step) if step else packed[step]
    collected = [None] * EXPERTS
    for step in ORDER:
        line = [arrived[step]] + [beside(arrived[step], turn) for turn in range(1, along)]
        line = line + [across(x) for x in line]
        outs = experts(line, expert_gate, expert_up, expert_down)
        others = [across(x) for x in outs[along:]]
        near = [add(own, other) for own, other in zip(outs[:along], others)]
        others = [beside(near[turn], turn) for turn in range(1, along)]
        reduced = add(near[0], *others)
        collected[step] = planes(reduced, step) if step else reduced

    def combined(base, steps, kind):
        return call(
            functools.partial(combine_kernel, along, steps),
            shape((local_rows, model_width), kind),
            (base, expert_choice.T, gate_weights.T, *[collected[step] for step in steps]),
            flops=2 * len(steps) * ROWS * local_rows * model_width,
            moved=8 * local_rows * model_width,
        )

    a, b, c, d = ORDER
    early = combined(residual, (a, b), f32)
    return combined(early, (c, d), bf16)


def solution(mesh):
    assert mesh.shape["dp"] == 2 and mesh.shape["expert"] % EXPERTS == 0
    in_specs = (
        P(("group", "expert", "dp"), None),
        P(("group", "expert", "dp"), None),
        P(("group", "expert", "dp"), None),
        P(),
        P("dp", None),
        P("dp", None),
        P("dp", None),
        P(),
        P(None, ("expert", "dp")),
        P(None, ("expert", "dp")),
        P(("expert", "dp"), None),
    )
    out_specs = P(("group", "expert", "dp"), None)

    return jax.shard_map(body, mesh=mesh, in_specs=in_specs, out_specs=out_specs, check_vma=False)
```

```python
import functools
import math

import jax
import jax.numpy as jnp
from jax import lax
from jax.experimental import pallas as pl
from jax.experimental.pallas import tpu as pltpu
from jax.sharding import PartitionSpec as P


HEAD_DIM = 128
EXPERTS = 4
CAP = 70
ROWS = -(-CAP // 8) * 8

HIDDEN_STEP = 256
DOWN_STEP = 256
ORDER = (0, 2, 1, 3)

epsilon = 1e-05
base_theta = 1000000.0
masked_score = -1e30

VMEM = pl.BlockSpec(memory_space=pltpu.VMEM)
f32 = jnp.float32
bf16 = jnp.bfloat16


def dot(a, b):
    return jnp.dot(a, b, preferred_element_type=f32)


def call(kernel, outs, operands, scratch=(), flops=0, moved=0, limit=16 << 20):
    return pl.pallas_call(
        kernel,
        out_shape=outs,
        in_specs=[VMEM] * len(operands),
        out_specs=jax.tree.map(lambda _: VMEM, outs),
        scratch_shapes=list(scratch),
        compiler_params=pltpu.CompilerParams(vmem_limit_bytes=limit),
        cost_estimate=pl.CostEstimate(flops=flops, bytes_accessed=moved, transcendentals=0),
    )(*operands)


def normalized(widened, gain):
    spread = jnp.mean(widened * widened, axis=-1, keepdims=True)
    return (widened * lax.rsqrt(spread + epsilon) * gain).astype(bf16)


def norm_kernel(tokens_ref, gain_ref, keep_ref, send_ref, whole_ref):
    half = keep_ref.shape[1]
    whole_ref[...] = normalized(tokens_ref[...].astype(f32), gain_ref[...])
    core = lax.axis_index("dp")
    keep_ref[...] = whole_ref[:, pl.ds(pl.multiple_of(core * half, half), half)]
    send_ref[...] = whole_ref[:, pl.ds(pl.multiple_of((1 - core) * half, half), half)]


def keyval_kernel(mine_ref, theirs_ref, weight_ref, keep_ref, send_ref):
    rows = jnp.concatenate([mine_ref[...], theirs_ref[...]], axis=0)
    width = keep_ref.shape[1] // 2
    core = lax.axis_index("dp")
    for out_ref, owner in ((send_ref, 1 - core), (keep_ref, core)):
        for part in range(2):
            start = pl.multiple_of((part * 2 + owner) * width, width)
            out_ref[:, part * width : (part + 1) * width] = dot(
                rows, weight_ref[:, pl.ds(start, width)]
            )


def query_kernel(mine_ref, theirs_ref, weight_ref, keep_ref, send_ref):
    rows = jnp.concatenate([mine_ref[...], theirs_ref[...]], axis=0)
    width = keep_ref.shape[1]
    step = min(512, width)
    core = lax.axis_index("dp")
    for out_ref, owner in ((send_ref, 1 - core), (keep_ref, core)):
        for offset in range(0, width, step):
            start = pl.multiple_of(owner * width + offset, step)
            out_ref[:, offset : offset + step] = dot(rows, weight_ref[:, pl.ds(start, step)])


def summed(keep_ref, came_ref, columns):
    half = keep_ref.shape[0] // 2
    came = came_ref[:, columns]
    return keep_ref[:, columns] + jnp.concatenate([came[half:], came[:half]], axis=0)


def turned(vectors, cosine, sine):
    return vectors * cosine + pltpu.roll(vectors, HEAD_DIM // 2, 1) * sine


def keyval_turn_kernel(keep_ref, came_ref, cosine_ref, sine_ref, out_ref):
    width = out_ref.shape[1]
    for start in range(0, width, HEAD_DIM):
        columns = slice(start, start + HEAD_DIM)
        total = summed(keep_ref, came_ref, columns)
        if start < width // 2:
            total = turned(total, cosine_ref[...], sine_ref[...])
        out_ref[:, columns] = total.astype(bf16)


def query_turn_kernel(keep_ref, came_ref, cosine_ref, sine_ref, out_ref):
    for head in range(out_ref.shape[0]):
        columns = slice(head * HEAD_DIM, (head + 1) * HEAD_DIM)
        total = summed(keep_ref, came_ref, columns)
        out_ref[head] = turned(total, cosine_ref[...], sine_ref[...]).astype(bf16)


def attention_kernel(places, along, first, last, query_ref, *refs):
    refs = list(refs)
    keyval_refs = [refs.pop(0) for _ in places]
    before = [] if first else [refs.pop(0) for _ in range(3)]
    weight_ref = refs.pop(0) if last else None
    after = [refs.pop(0) for _ in range(2 if last else 3)]
    score_ref = refs.pop(0)
    context_ref = refs.pop(0) if last else None
    heads, rows, _ = query_ref.shape
    half = rows // 2
    shared = keyval_refs[0].shape[1] // (2 * HEAD_DIM)
    sharing = heads // shared
    core = lax.axis_index("dp")
    chip = lax.axis_index("expert")
    plane, place = chip // along, chip % along

    def position(shape, axis):
        row = lax.broadcasted_iota(jnp.int32, shape, axis)
        return jnp.where(core == 0, row, jnp.where(row < half, row + half, row - half))

    if first:
        own_visible = position((rows, rows), 1) <= position((rows, rows), 0)
    seen = []
    for back, turn in places:
        if back == 0:
            seen.append((place ^ turn) < place)
        else:
            seen.append(plane >= back)
    factor = HEAD_DIM ** (-0.5) * math.log2(math.e)

    def one_group(group, _):
        key_columns = pl.ds(pl.multiple_of(group * HEAD_DIM, HEAD_DIM), HEAD_DIM)
        value_columns = pl.ds(
            pl.multiple_of((shared + group) * HEAD_DIM, HEAD_DIM), HEAD_DIM
        )

        def one_head(member):
            head = group * sharing + member
            query = query_ref[head]
            highest = None
            for index, keyval_ref in enumerate(keyval_refs):
                score = lax.dot_general(
                    query,
                    keyval_ref[:, key_columns],
                    (((1,), (1,)), ((), ())),
                    preferred_element_type=f32,
                ) * factor
                own = first and index == 0
                if own:
                    score = jnp.where(own_visible, score, masked_score)
                score_ref[member, :, index * rows : (index + 1) * rows] = score
                most = score[:, :HEAD_DIM]
                for start in range(HEAD_DIM, rows, HEAD_DIM):
                    most = jnp.maximum(most, score[:, start : start + HEAD_DIM])
                if not own:
                    most = jnp.where(seen[index], most, masked_score)
                highest = most if highest is None else jnp.maximum(highest, most)
            highest = jnp.broadcast_to(
                jnp.max(highest, axis=-1, keepdims=True), (rows, HEAD_DIM)
            )
            if first:
                totals = jnp.zeros((rows, HEAD_DIM), f32)
                mixed = jnp.zeros((rows, HEAD_DIM), f32)
            else:
                earlier = before[0][head]
                highest = jnp.maximum(highest, earlier)
                shrink = jnp.exp2(earlier - highest)
                totals = before[1][head] * shrink
                mixed = before[2][head] * shrink
            for index, keyval_ref in enumerate(keyval_refs):
                ceiling = highest
                if not (first and index == 0):
                    ceiling = jnp.where(seen[index], highest, -masked_score)
                probs = []
                for start in range(index * rows, (index + 1) * rows, HEAD_DIM):
                    expo = jnp.exp2(score_ref[member, :, start : start + HEAD_DIM] - ceiling)
                    totals = totals + expo
                    probs.append(expo.astype(bf16))
                mixed = mixed + dot(jnp.concatenate(probs, axis=1), keyval_ref[:, value_columns])
            if last:
                total = jnp.sum(totals, axis=-1, keepdims=True)
                context_ref[head] = (mixed / total).astype(bf16)
            else:
                after[0][head] = highest
                after[1][head] = totals
                after[2][head] = mixed

        for member in range(sharing):
            one_head(member)
        return 0

    lax.fori_loop(0, shared, one_group, 0)

    if last:
        send_ref, keep_ref = after
        context = jnp.concatenate([context_ref[head] for head in range(heads)], axis=1)
        step = min(512, send_ref.shape[1])
        for start in range(0, send_ref.shape[1], step):
            columns = slice(start, start + step)
            out = dot(context, weight_ref[:, columns])
            keep_ref[:, columns] = out[:half]
            send_ref[:, columns] = out[half:].astype(bf16)


def as_columns(rows_ref):
    count = rows_ref.shape[1]
    same = (
        lax.broadcasted_iota(jnp.int32, (count, count), 0)
        == lax.broadcasted_iota(jnp.int32, (count, count), 1)
    )
    return lax.dot_general(
        same.astype(f32),
        rows_ref[...].astype(f32),
        (((1,), (1,)), ((), ())),
        precision=lax.Precision.HIGHEST,
        preferred_element_type=f32,
    )


def placed(choice, plane):
    rows = choice.shape[0]
    first, second = choice[:, 0:1], choice[:, 1:2]
    lane = lax.broadcasted_iota(jnp.int32, (rows, 128), 1)
    goes = jnp.zeros((rows, 128), jnp.bool_)
    for step in range(EXPERTS):
        expert = plane ^ step
        goes = goes | ((lane == step) & ((first == expert) | (second == expert)))
    earlier = (
        lax.broadcasted_iota(jnp.int32, (rows, rows), 1)
        < lax.broadcasted_iota(jnp.int32, (rows, rows), 0)
    )
    slots = dot(earlier.astype(bf16), goes.astype(bf16)).astype(jnp.int32)
    slots = jnp.where(goes, slots, -1)
    return [
        (lane[:, :ROWS] == slots[:, step : step + 1]).astype(bf16) for step in range(EXPERTS)
    ]


def pack_kernel(along, keep_ref, came_ref, tokens_ref, gain_ref, choice_ref, residual_ref, *out_refs):
    attention = keep_ref[...] + came_ref[...].astype(f32)
    residual = (tokens_ref[...].astype(f32) + attention).astype(bf16)
    residual_ref[...] = residual
    mixed_in = normalized(residual.astype(f32), gain_ref[...])
    plane = lax.axis_index("expert") // along
    choice = as_columns(choice_ref).astype(jnp.int32)
    for out_ref, routing in zip(out_refs, placed(choice, plane)):
        out_ref[...] = lax.dot_general(
            routing, mixed_in, (((0,), (0,)), ((), ())), preferred_element_type=f32
        ).astype(bf16)


def fetch_kernel(parts, from_ref, to_ref, sem):
    rows = from_ref.shape[0] // parts
    copies = []
    for part in range(parts):
        block = pl.ds(part * rows, rows)
        copies.append(
            pltpu.make_async_copy(from_ref.at[block], to_ref.at[block], sem.at[part])
        )
    for copy in copies:
        copy.start()
    for copy in copies:
        copy.wait()


def fetched(weight):
    parts = 4
    return pl.pallas_call(
        functools.partial(fetch_kernel, parts),
        out_shape=jax.ShapeDtypeStruct(weight.shape, weight.dtype),
        in_specs=[pl.BlockSpec(memory_space=pltpu.HBM)],
        out_specs=VMEM,
        scratch_shapes=[pltpu.SemaphoreType.DMA((parts,))],
        compiler_params=pltpu.CompilerParams(vmem_limit_bytes=2 << 20),
        cost_estimate=pl.CostEstimate(
            flops=0, bytes_accessed=4 * weight.size, transcendentals=0
        ),
        name="fetch",
    )(weight)


def expert_kernel(count, gate_ref, up_ref, down_ref, *refs):
    row_refs, out_refs, hidden_ref = refs[:count], refs[count : 2 * count], refs[2 * count]
    rows = jnp.concatenate([row_ref[...] for row_ref in row_refs], axis=0)
    for start in range(0, hidden_ref.shape[1], HIDDEN_STEP):
        columns = slice(start, start + HIDDEN_STEP)
        gate = dot(rows, gate_ref[:, columns])
        upward = dot(rows, up_ref[:, columns])
        hidden_ref[:, columns] = (gate / (1.0 + jnp.exp(-gate)) * upward).astype(bf16)
    hidden = hidden_ref[...]
    for start in range(0, down_ref.shape[1], DOWN_STEP):
        columns = slice(start, start + DOWN_STEP)
        out = dot(hidden, down_ref[:, columns]).astype(bf16)
        for index, out_ref in enumerate(out_refs):
            out_ref[:, columns] = out[index * ROWS : (index + 1) * ROWS]


def experts(rows, expert_gate, expert_up, expert_down):
    width, hidden = expert_gate.shape
    count = len(rows)
    return call(
        functools.partial(expert_kernel, count),
        [jax.ShapeDtypeStruct((ROWS, width), bf16)] * count,
        (expert_gate, expert_up, expert_down, *rows),
        scratch=[pltpu.VMEM((count * ROWS, hidden), bf16)],
        flops=6 * count * ROWS * width * hidden,
        moved=6 * width * hidden,
        limit=12 << 20,
    )


def combine_kernel(along, steps, base_ref, choice_ref, weight_ref, *refs):
    row_refs, out_ref = refs[:-1], refs[-1]
    plane = lax.axis_index("expert") // along
    choice = as_columns(choice_ref).astype(jnp.int32)
    weights = as_columns(weight_ref)
    total = base_ref[...].astype(f32)
    routings = placed(choice, plane)
    for step, row_ref in zip(steps, row_refs):
        expert = plane ^ step
        weight = jnp.sum(jnp.where(choice == expert, weights, 0.0), axis=1, keepdims=True)
        total = total + weight * dot(routings[step], row_ref[...])
    out_ref[...] = total.astype(out_ref.dtype)


def add(*terms):
    return sum(term.astype(f32) for term in terms).astype(bf16)


def body(
    tokens,
    expert_choice,
    gate_weights,
    attention_gain,
    query_weight,
    key_value_weight,
    output_weight,
    feedforward_gain,
    expert_gate,
    expert_up,
    expert_down,
):
    local_rows, model_width = tokens.shape
    share = query_weight.shape[0]
    cores = lax.axis_size("dp")
    chips = lax.axis_size("expert")
    along = chips // EXPERTS
    query_width = query_weight.shape[1] // cores
    keyval_width = key_value_weight.shape[1] // cores
    heads = query_width // HEAD_DIM
    sharing = query_weight.shape[1] * 2 // key_value_weight.shape[1]
    pair_rows = local_rows * cores
    chip = lax.axis_index("expert")
    core = lax.axis_index("dp")

    def across(x):
        return lax.ppermute(x, "dp", [(i, i ^ 1) for i in range(cores)])

    def beside(x, turn):
        return lax.ppermute(x, "expert", [(i, i ^ turn) for i in range(chips)])

    def upward(x):
        return lax.ppermute(x, "expert", [(i, (i + along) % chips) for i in range(chips)])

    def planes(x, step):
        return lax.ppermute(x, "expert", [(i, i ^ (step * along)) for i in range(chips)])

    order = jnp.arange(pair_rows, dtype=jnp.int32)
    order = (order + core * local_rows) % pair_rows
    positions = chip * pair_rows + order
    halfway = HEAD_DIM // 2
    powers = jnp.arange(halfway, dtype=f32) * (2.0 / HEAD_DIM)
    inverse = base_theta ** (-powers)
    angles = positions.astype(f32)[:, None] * inverse[None, :]
    cosine, sine = jnp.cos(angles), jnp.sin(angles)
    cosine = jnp.concatenate([cosine, cosine], axis=1)
    sine = jnp.concatenate([-sine, sine], axis=1)

    shape = jax.ShapeDtypeStruct
    mine, outgoing = call(
        norm_kernel,
        [shape((local_rows, share), bf16)] * 2,
        (tokens, attention_gain.reshape(1, -1)),
        scratch=[pltpu.VMEM((local_rows, model_width), bf16)],
        flops=8 * local_rows * model_width,
        moved=4 * local_rows * model_width,
    )
    theirs = across(outgoing)
    key_value_weight = fetched(key_value_weight)
    keyval_keep, keyval_send = call(
        keyval_kernel,
        [shape((pair_rows, keyval_width), f32)] * 2,
        (mine, theirs, key_value_weight),
        flops=4 * pair_rows * share * keyval_width,
        moved=4 * share * keyval_width,
    )
    keyval_came = across(keyval_send)
    query_keep, query_send = call(
        query_kernel,
        [shape((pair_rows, query_width), f32)] * 2,
        (mine, theirs, query_weight),
        flops=4 * pair_rows * share * query_width,
        moved=4 * share * query_width,
    )
    query_came = across(query_send)
    keyval = call(
        keyval_turn_kernel,
        shape((pair_rows, keyval_width), bf16),
        (keyval_keep, keyval_came, cosine, sine),
        flops=8 * pair_rows * keyval_width,
        moved=10 * pair_rows * keyval_width,
    )
    queries = call(
        query_turn_kernel,
        shape((heads, pair_rows, HEAD_DIM), bf16),
        (query_keep, query_came, cosine, sine),
        flops=8 * pair_rows * query_width,
        moved=10 * pair_rows * query_width,
    )
    parts, part = [], []
    line = keyval
    for back in range(EXPERTS):
        if back:
            line = upward(line)
        part.append((line, (back, 0)))
        if back:
            parts.append(part)
            part = []
        part += [(beside(line, turn), (back, turn)) for turn in range(1, along)]
    parts.append(part)
    state = []
    for index, part in enumerate(parts):
        blocks, places = zip(*part) if part else ((), ())
        last = index == len(parts) - 1
        outs = [shape((heads, pair_rows, HEAD_DIM), f32)] * 3
        scratch = [
            pltpu.VMEM((sharing, pair_rows, pair_rows * max(1, len(blocks))), f32)
        ]
        if last:
            outs = [shape((local_rows, model_width), bf16), shape((local_rows, model_width), f32)]
            scratch.append(pltpu.VMEM((heads, pair_rows, HEAD_DIM), bf16))
        state = call(
            functools.partial(attention_kernel, places, along, index == 0, last),
            outs,
            (queries, *blocks, *state, *([output_weight] if last else [])),
            scratch=scratch,
            flops=4 * pair_rows * pair_rows * len(blocks) * query_width
            + 2 * pair_rows * query_width * model_width * last,
            moved=8 * pair_rows * query_width,
            limit=14 << 20,
        )
    attention_send, attention_keep = state
    attention_came = across(attention_send)
    residual, *packed = call(
        functools.partial(pack_kernel, along),
        [shape((local_rows, model_width), bf16)] + [shape((ROWS, model_width), bf16)] * EXPERTS,
        (
            attention_keep,
            attention_came,
            tokens,
            feedforward_gain.reshape(1, -1),
            expert_choice.T,
        ),
        flops=2 * EXPERTS * ROWS * local_rows * model_width,
        moved=12 * local_rows * model_width,
    )
    expert_gate = fetched(expert_gate)
    expert_up = fetched(expert_up)
    expert_down = fetched(expert_down)
    arrived = {}
    for step in ORDER:
        arrived[step] = planes(packed[step], step) if step else packed[step]
    collected = [None] * EXPERTS
    for step in ORDER:
        line = [arrived[step]] + [beside(arrived[step], turn) for turn in range(1, along)]
        line = line + [across(x) for x in line]
        outs = experts(line, expert_gate, expert_up, expert_down)
        others = [across(x) for x in outs[along:]]
        near = [add(own, other) for own, other in zip(outs[:along], others)]
        others = [beside(near[turn], turn) for turn in range(1, along)]
        reduced = add(near[0], *others)
        collected[step] = planes(reduced, step) if step else reduced

    def combined(base, steps, kind):
        return call(
            functools.partial(combine_kernel, along, steps),
            shape((local_rows, model_width), kind),
            (base, expert_choice.T, gate_weights.T, *[collected[step] for step in steps]),
            flops=2 * len(steps) * ROWS * local_rows * model_width,
            moved=8 * local_rows * model_width,
        )

    a, b, c, d = ORDER
    early = combined(residual, (a, b), f32)
    return combined(early, (c, d), bf16)


def solution(mesh):
    assert mesh.shape["dp"] == 2 and mesh.shape["expert"] % EXPERTS == 0
    in_specs = (
        P(("group", "expert", "dp"), None),
        P(("group", "expert", "dp"), None),
        P(("group", "expert", "dp"), None),
        P(),
        P("dp", None),
        P("dp", None),
        P("dp", None),
        P(),
        P(None, ("expert", "dp")),
        P(None, ("expert", "dp")),
        P(("expert", "dp"), None),
    )
    out_specs = P(("group", "expert", "dp"), None)

    return jax.shard_map(body, mesh=mesh, in_specs=in_specs, out_specs=out_specs, check_vma=False)
```

```python
import functools
import math

import jax
import jax.numpy as jnp
from jax import lax
from jax.experimental import pallas as pl
from jax.experimental.pallas import tpu as pltpu
from jax.sharding import PartitionSpec as P


HEAD_DIM = 128
EXPERTS = 4
CAP = 70
ROWS = -(-CAP // 8) * 8

HIDDEN_STEP = 256
DOWN_STEP = 256
ORDER = (0, 1, 2, 3)

epsilon = 1e-05
base_theta = 1000000.0
masked_score = -1e30

VMEM = pl.BlockSpec(memory_space=pltpu.VMEM)
f32 = jnp.float32
bf16 = jnp.bfloat16


def dot(a, b):
    return jnp.dot(a, b, preferred_element_type=f32)


def call(kernel, outs, operands, scratch=(), flops=0, moved=0, limit=16 << 20):
    return pl.pallas_call(
        kernel,
        out_shape=outs,
        in_specs=[VMEM] * len(operands),
        out_specs=jax.tree.map(lambda _: VMEM, outs),
        scratch_shapes=list(scratch),
        compiler_params=pltpu.CompilerParams(vmem_limit_bytes=limit),
        cost_estimate=pl.CostEstimate(flops=flops, bytes_accessed=moved, transcendentals=0),
    )(*operands)


def normalized(widened, gain):
    spread = jnp.mean(widened * widened, axis=-1, keepdims=True)
    return (widened * lax.rsqrt(spread + epsilon) * gain).astype(bf16)


def norm_kernel(tokens_ref, gain_ref, keep_ref, send_ref, whole_ref):
    half = keep_ref.shape[1]
    whole_ref[...] = normalized(tokens_ref[...].astype(f32), gain_ref[...])
    core = lax.axis_index("dp")
    keep_ref[...] = whole_ref[:, pl.ds(pl.multiple_of(core * half, half), half)]
    send_ref[...] = whole_ref[:, pl.ds(pl.multiple_of((1 - core) * half, half), half)]


def keyval_kernel(mine_ref, theirs_ref, weight_ref, keep_ref, send_ref):
    rows = jnp.concatenate([mine_ref[...], theirs_ref[...]], axis=0)
    width = keep_ref.shape[1] // 2
    core = lax.axis_index("dp")
    for out_ref, owner in ((send_ref, 1 - core), (keep_ref, core)):
        for part in range(2):
            start = pl.multiple_of((part * 2 + owner) * width, width)
            out_ref[:, part * width : (part + 1) * width] = dot(
                rows, weight_ref[:, pl.ds(start, width)]
            )


def query_kernel(mine_ref, theirs_ref, weight_ref, keep_ref, send_ref):
    rows = jnp.concatenate([mine_ref[...], theirs_ref[...]], axis=0)
    width = keep_ref.shape[1]
    step = min(512, width)
    core = lax.axis_index("dp")
    for out_ref, owner in ((send_ref, 1 - core), (keep_ref, core)):
        for offset in range(0, width, step):
            start = pl.multiple_of(owner * width + offset, step)
            out_ref[:, offset : offset + step] = dot(rows, weight_ref[:, pl.ds(start, step)])


def summed(keep_ref, came_ref, columns):
    half = keep_ref.shape[0] // 2
    came = came_ref[:, columns]
    return keep_ref[:, columns] + jnp.concatenate([came[half:], came[:half]], axis=0)


def turned(vectors, cosine, sine):
    return vectors * cosine + pltpu.roll(vectors, HEAD_DIM // 2, 1) * sine


def keyval_turn_kernel(keep_ref, came_ref, cosine_ref, sine_ref, out_ref):
    width = out_ref.shape[1]
    for start in range(0, width, HEAD_DIM):
        columns = slice(start, start + HEAD_DIM)
        total = summed(keep_ref, came_ref, columns)
        if start < width // 2:
            total = turned(total, cosine_ref[...], sine_ref[...])
        out_ref[:, columns] = total.astype(bf16)


def query_turn_kernel(keep_ref, came_ref, cosine_ref, sine_ref, out_ref):
    for head in range(out_ref.shape[0]):
        columns = slice(head * HEAD_DIM, (head + 1) * HEAD_DIM)
        total = summed(keep_ref, came_ref, columns)
        out_ref[head] = turned(total, cosine_ref[...], sine_ref[...]).astype(bf16)


def attention_kernel(places, along, first, last, query_ref, *refs):
    refs = list(refs)
    keyval_refs = [refs.pop(0) for _ in places]
    before = [] if first else [refs.pop(0) for _ in range(3)]
    weight_ref = refs.pop(0) if last else None
    after = [refs.pop(0) for _ in range(2 if last else 3)]
    score_ref = refs.pop(0)
    context_ref = refs.pop(0) if last else None
    heads, rows, _ = query_ref.shape
    half = rows // 2
    shared = keyval_refs[0].shape[1] // (2 * HEAD_DIM)
    sharing = heads // shared
    core = lax.axis_index("dp")
    chip = lax.axis_index("expert")
    plane, place = chip // along, chip % along

    def position(shape, axis):
        row = lax.broadcasted_iota(jnp.int32, shape, axis)
        return jnp.where(core == 0, row, jnp.where(row < half, row + half, row - half))

    if first:
        own_visible = position((rows, rows), 1) <= position((rows, rows), 0)
    seen = []
    for back, turn in places:
        if back == 0:
            seen.append((place ^ turn) < place)
        else:
            seen.append(plane >= back)
    factor = HEAD_DIM ** (-0.5) * math.log2(math.e)

    def one_group(group, _):
        key_columns = pl.ds(pl.multiple_of(group * HEAD_DIM, HEAD_DIM), HEAD_DIM)
        value_columns = pl.ds(
            pl.multiple_of((shared + group) * HEAD_DIM, HEAD_DIM), HEAD_DIM
        )

        def one_head(member):
            head = group * sharing + member
            query = query_ref[head]
            highest = None
            for index, keyval_ref in enumerate(keyval_refs):
                score = lax.dot_general(
                    query,
                    keyval_ref[:, key_columns],
                    (((1,), (1,)), ((), ())),
                    preferred_element_type=f32,
                ) * factor
                own = first and index == 0
                if own:
                    score = jnp.where(own_visible, score, masked_score)
                score_ref[member, :, index * rows : (index + 1) * rows] = score
                most = score[:, :HEAD_DIM]
                for start in range(HEAD_DIM, rows, HEAD_DIM):
                    most = jnp.maximum(most, score[:, start : start + HEAD_DIM])
                if not own:
                    most = jnp.where(seen[index], most, masked_score)
                highest = most if highest is None else jnp.maximum(highest, most)
            highest = jnp.broadcast_to(
                jnp.max(highest, axis=-1, keepdims=True), (rows, HEAD_DIM)
            )
            if first:
                totals = jnp.zeros((rows, HEAD_DIM), f32)
                mixed = jnp.zeros((rows, HEAD_DIM), f32)
            else:
                earlier = before[0][head]
                highest = jnp.maximum(highest, earlier)
                shrink = jnp.exp2(earlier - highest)
                totals = before[1][head] * shrink
                mixed = before[2][head] * shrink
            for index, keyval_ref in enumerate(keyval_refs):
                ceiling = highest
                if not (first and index == 0):
                    ceiling = jnp.where(seen[index], highest, -masked_score)
                probs = []
                for start in range(index * rows, (index + 1) * rows, HEAD_DIM):
                    expo = jnp.exp2(score_ref[member, :, start : start + HEAD_DIM] - ceiling)
                    totals = totals + expo
                    probs.append(expo.astype(bf16))
                mixed = mixed + dot(jnp.concatenate(probs, axis=1), keyval_ref[:, value_columns])
            if last:
                total = jnp.sum(totals, axis=-1, keepdims=True)
                context_ref[head] = (mixed / total).astype(bf16)
            else:
                after[0][head] = highest
                after[1][head] = totals
                after[2][head] = mixed

        for member in range(sharing):
            one_head(member)
        return 0

    lax.fori_loop(0, shared, one_group, 0)

    if last:
        send_ref, keep_ref = after
        context = jnp.concatenate([context_ref[head] for head in range(heads)], axis=1)
        step = min(512, send_ref.shape[1])
        for start in range(0, send_ref.shape[1], step):
            columns = slice(start, start + step)
            out = dot(context, weight_ref[:, columns])
            keep_ref[:, columns] = out[:half]
            send_ref[:, columns] = out[half:].astype(bf16)


def as_columns(rows_ref):
    count = rows_ref.shape[1]
    same = (
        lax.broadcasted_iota(jnp.int32, (count, count), 0)
        == lax.broadcasted_iota(jnp.int32, (count, count), 1)
    )
    return lax.dot_general(
        same.astype(f32),
        rows_ref[...].astype(f32),
        (((1,), (1,)), ((), ())),
        precision=lax.Precision.HIGHEST,
        preferred_element_type=f32,
    )


def placed(choice, plane):
    rows = choice.shape[0]
    first, second = choice[:, 0:1], choice[:, 1:2]
    lane = lax.broadcasted_iota(jnp.int32, (rows, 128), 1)
    goes = jnp.zeros((rows, 128), jnp.bool_)
    for step in range(EXPERTS):
        expert = plane ^ step
        goes = goes | ((lane == step) & ((first == expert) | (second == expert)))
    earlier = (
        lax.broadcasted_iota(jnp.int32, (rows, rows), 1)
        < lax.broadcasted_iota(jnp.int32, (rows, rows), 0)
    )
    slots = dot(earlier.astype(bf16), goes.astype(bf16)).astype(jnp.int32)
    slots = jnp.where(goes, slots, -1)
    return [
        (lane[:, :ROWS] == slots[:, step : step + 1]).astype(bf16) for step in range(EXPERTS)
    ]


def pack_kernel(along, keep_ref, came_ref, tokens_ref, gain_ref, choice_ref, residual_ref, *out_refs):
    attention = keep_ref[...] + came_ref[...].astype(f32)
    residual = (tokens_ref[...].astype(f32) + attention).astype(bf16)
    residual_ref[...] = residual
    mixed_in = normalized(residual.astype(f32), gain_ref[...])
    plane = lax.axis_index("expert") // along
    choice = as_columns(choice_ref).astype(jnp.int32)
    for out_ref, routing in zip(out_refs, placed(choice, plane)):
        out_ref[...] = lax.dot_general(
            routing, mixed_in, (((0,), (0,)), ((), ())), preferred_element_type=f32
        ).astype(bf16)


def fetch_kernel(parts, from_ref, to_ref, sem):
    rows = from_ref.shape[0] // parts
    copies = []
    for part in range(parts):
        block = pl.ds(part * rows, rows)
        copies.append(
            pltpu.make_async_copy(from_ref.at[block], to_ref.at[block], sem.at[part])
        )
    for copy in copies:
        copy.start()
    for copy in copies:
        copy.wait()


def fetched(weight):
    parts = 4
    return pl.pallas_call(
        functools.partial(fetch_kernel, parts),
        out_shape=jax.ShapeDtypeStruct(weight.shape, weight.dtype),
        in_specs=[pl.BlockSpec(memory_space=pltpu.HBM)],
        out_specs=VMEM,
        scratch_shapes=[pltpu.SemaphoreType.DMA((parts,))],
        compiler_params=pltpu.CompilerParams(vmem_limit_bytes=2 << 20),
        cost_estimate=pl.CostEstimate(
            flops=0, bytes_accessed=4 * weight.size, transcendentals=0
        ),
        name="fetch",
    )(weight)


def expert_kernel(count, gate_ref, up_ref, down_ref, *refs):
    row_refs, out_refs, hidden_ref = refs[:count], refs[count : 2 * count], refs[2 * count]
    rows = jnp.concatenate([row_ref[...] for row_ref in row_refs], axis=0)
    for start in range(0, hidden_ref.shape[1], HIDDEN_STEP):
        columns = slice(start, start + HIDDEN_STEP)
        gate = dot(rows, gate_ref[:, columns])
        upward = dot(rows, up_ref[:, columns])
        hidden_ref[:, columns] = (gate / (1.0 + jnp.exp(-gate)) * upward).astype(bf16)
    hidden = hidden_ref[...]
    for start in range(0, down_ref.shape[1], DOWN_STEP):
        columns = slice(start, start + DOWN_STEP)
        out = dot(hidden, down_ref[:, columns]).astype(bf16)
        for index, out_ref in enumerate(out_refs):
            out_ref[:, columns] = out[index * ROWS : (index + 1) * ROWS]


def experts(rows, expert_gate, expert_up, expert_down):
    width, hidden = expert_gate.shape
    count = len(rows)
    return call(
        functools.partial(expert_kernel, count),
        [jax.ShapeDtypeStruct((ROWS, width), bf16)] * count,
        (expert_gate, expert_up, expert_down, *rows),
        scratch=[pltpu.VMEM((count * ROWS, hidden), bf16)],
        flops=6 * count * ROWS * width * hidden,
        moved=6 * width * hidden,
        limit=12 << 20,
    )


def combine_kernel(along, steps, base_ref, choice_ref, weight_ref, *refs):
    row_refs, out_ref = refs[:-1], refs[-1]
    plane = lax.axis_index("expert") // along
    choice = as_columns(choice_ref).astype(jnp.int32)
    weights = as_columns(weight_ref)
    total = base_ref[...].astype(f32)
    routings = placed(choice, plane)
    for step, row_ref in zip(steps, row_refs):
        expert = plane ^ step
        weight = jnp.sum(jnp.where(choice == expert, weights, 0.0), axis=1, keepdims=True)
        total = total + weight * dot(routings[step], row_ref[...])
    out_ref[...] = total.astype(out_ref.dtype)


def add(*terms):
    return sum(term.astype(f32) for term in terms).astype(bf16)


def body(
    tokens,
    expert_choice,
    gate_weights,
    attention_gain,
    query_weight,
    key_value_weight,
    output_weight,
    feedforward_gain,
    expert_gate,
    expert_up,
    expert_down,
):
    local_rows, model_width = tokens.shape
    share = query_weight.shape[0]
    cores = lax.axis_size("dp")
    chips = lax.axis_size("expert")
    along = chips // EXPERTS
    query_width = query_weight.shape[1] // cores
    keyval_width = key_value_weight.shape[1] // cores
    heads = query_width // HEAD_DIM
    sharing = query_weight.shape[1] * 2 // key_value_weight.shape[1]
    pair_rows = local_rows * cores
    chip = lax.axis_index("expert")
    core = lax.axis_index("dp")

    def across(x):
        return lax.ppermute(x, "dp", [(i, i ^ 1) for i in range(cores)])

    def beside(x, turn):
        return lax.ppermute(x, "expert", [(i, i ^ turn) for i in range(chips)])

    def upward(x):
        return lax.ppermute(x, "expert", [(i, (i + along) % chips) for i in range(chips)])

    def planes(x, step):
        return lax.ppermute(x, "expert", [(i, i ^ (step * along)) for i in range(chips)])

    order = jnp.arange(pair_rows, dtype=jnp.int32)
    order = (order + core * local_rows) % pair_rows
    positions = chip * pair_rows + order
    halfway = HEAD_DIM // 2
    powers = jnp.arange(halfway, dtype=f32) * (2.0 / HEAD_DIM)
    inverse = base_theta ** (-powers)
    angles = positions.astype(f32)[:, None] * inverse[None, :]
    cosine, sine = jnp.cos(angles), jnp.sin(angles)
    cosine = jnp.concatenate([cosine, cosine], axis=1)
    sine = jnp.concatenate([-sine, sine], axis=1)

    shape = jax.ShapeDtypeStruct
    mine, outgoing = call(
        norm_kernel,
        [shape((local_rows, share), bf16)] * 2,
        (tokens, attention_gain.reshape(1, -1)),
        scratch=[pltpu.VMEM((local_rows, model_width), bf16)],
        flops=8 * local_rows * model_width,
        moved=4 * local_rows * model_width,
    )
    theirs = across(outgoing)
    key_value_weight = fetched(key_value_weight)
    keyval_keep, keyval_send = call(
        keyval_kernel,
        [shape((pair_rows, keyval_width), f32)] * 2,
        (mine, theirs, key_value_weight),
        flops=4 * pair_rows * share * keyval_width,
        moved=4 * share * keyval_width,
    )
    keyval_came = across(keyval_send)
    query_keep, query_send = call(
        query_kernel,
        [shape((pair_rows, query_width), f32)] * 2,
        (mine, theirs, query_weight),
        flops=4 * pair_rows * share * query_width,
        moved=4 * share * query_width,
    )
    query_came = across(query_send)
    keyval = call(
        keyval_turn_kernel,
        shape((pair_rows, keyval_width), bf16),
        (keyval_keep, keyval_came, cosine, sine),
        flops=8 * pair_rows * keyval_width,
        moved=10 * pair_rows * keyval_width,
    )
    queries = call(
        query_turn_kernel,
        shape((heads, pair_rows, HEAD_DIM), bf16),
        (query_keep, query_came, cosine, sine),
        flops=8 * pair_rows * query_width,
        moved=10 * pair_rows * query_width,
    )
    parts, part = [], []
    line = keyval
    for back in range(EXPERTS):
        if back:
            line = upward(line)
        part.append((line, (back, 0)))
        if back:
            parts.append(part)
            part = []
        part += [(beside(line, turn), (back, turn)) for turn in range(1, along)]
    parts.append(part)
    state = []
    for index, part in enumerate(parts):
        blocks, places = zip(*part) if part else ((), ())
        last = index == len(parts) - 1
        outs = [shape((heads, pair_rows, HEAD_DIM), f32)] * 3
        scratch = [
            pltpu.VMEM((sharing, pair_rows, pair_rows * max(1, len(blocks))), f32)
        ]
        if last:
            outs = [shape((local_rows, model_width), bf16), shape((local_rows, model_width), f32)]
            scratch.append(pltpu.VMEM((heads, pair_rows, HEAD_DIM), bf16))
        state = call(
            functools.partial(attention_kernel, places, along, index == 0, last),
            outs,
            (queries, *blocks, *state, *([output_weight] if last else [])),
            scratch=scratch,
            flops=4 * pair_rows * pair_rows * len(blocks) * query_width
            + 2 * pair_rows * query_width * model_width * last,
            moved=8 * pair_rows * query_width,
            limit=14 << 20,
        )
    attention_send, attention_keep = state
    attention_came = across(attention_send)
    residual, *packed = call(
        functools.partial(pack_kernel, along),
        [shape((local_rows, model_width), bf16)] + [shape((ROWS, model_width), bf16)] * EXPERTS,
        (
            attention_keep,
            attention_came,
            tokens,
            feedforward_gain.reshape(1, -1),
            expert_choice.T,
        ),
        flops=2 * EXPERTS * ROWS * local_rows * model_width,
        moved=12 * local_rows * model_width,
    )
    expert_gate = fetched(expert_gate)
    expert_up = fetched(expert_up)
    expert_down = fetched(expert_down)
    arrived = {}
    for step in ORDER:
        arrived[step] = planes(packed[step], step) if step else packed[step]
    collected = [None] * EXPERTS
    for step in ORDER:
        line = [arrived[step]] + [beside(arrived[step], turn) for turn in range(1, along)]
        line = line + [across(x) for x in line]
        outs = experts(line, expert_gate, expert_up, expert_down)
        others = [across(x) for x in outs[along:]]
        near = [add(own, other) for own, other in zip(outs[:along], others)]
        others = [beside(near[turn], turn) for turn in range(1, along)]
        reduced = add(near[0], *others)
        collected[step] = planes(reduced, step) if step else reduced

    def combined(base, steps, kind):
        return call(
            functools.partial(combine_kernel, along, steps),
            shape((local_rows, model_width), kind),
            (base, expert_choice.T, gate_weights.T, *[collected[step] for step in steps]),
            flops=2 * len(steps) * ROWS * local_rows * model_width,
            moved=8 * local_rows * model_width,
        )

    a, b, c, d = ORDER
    early = combined(residual, (a, c), f32)
    return combined(early, (b, d), bf16)


def solution(mesh):
    assert mesh.shape["dp"] == 2 and mesh.shape["expert"] % EXPERTS == 0
    in_specs = (
        P(("group", "expert", "dp"), None),
        P(("group", "expert", "dp"), None),
        P(("group", "expert", "dp"), None),
        P(),
        P("dp", None),
        P("dp", None),
        P("dp", None),
        P(),
        P(None, ("expert", "dp")),
        P(None, ("expert", "dp")),
        P(("expert", "dp"), None),
    )
    out_specs = P(("group", "expert", "dp"), None)

    return jax.shard_map(body, mesh=mesh, in_specs=in_specs, out_specs=out_specs, check_vma=False)
```

```python
import functools
import math

import jax
import jax.numpy as jnp
from jax import lax
from jax.experimental import pallas as pl
from jax.experimental.pallas import tpu as pltpu
from jax.sharding import PartitionSpec as P


HEAD_DIM = 128
EXPERTS = 4
CAP = 70
ROWS = -(-CAP // 8) * 8

HIDDEN_STEP = 256
DOWN_STEP = 256
ORDER = (0, 2, 3, 1)

epsilon = 1e-05
base_theta = 1000000.0
masked_score = -1e30

VMEM = pl.BlockSpec(memory_space=pltpu.VMEM)
f32 = jnp.float32
bf16 = jnp.bfloat16


def dot(a, b):
    return jnp.dot(a, b, preferred_element_type=f32)


def call(kernel, outs, operands, scratch=(), flops=0, moved=0, limit=16 << 20):
    return pl.pallas_call(
        kernel,
        out_shape=outs,
        in_specs=[VMEM] * len(operands),
        out_specs=jax.tree.map(lambda _: VMEM, outs),
        scratch_shapes=list(scratch),
        compiler_params=pltpu.CompilerParams(vmem_limit_bytes=limit),
        cost_estimate=pl.CostEstimate(flops=flops, bytes_accessed=moved, transcendentals=0),
    )(*operands)


def normalized(widened, gain):
    spread = jnp.mean(widened * widened, axis=-1, keepdims=True)
    return (widened * lax.rsqrt(spread + epsilon) * gain).astype(bf16)


def norm_kernel(tokens_ref, gain_ref, keep_ref, send_ref, whole_ref):
    half = keep_ref.shape[1]
    whole_ref[...] = normalized(tokens_ref[...].astype(f32), gain_ref[...])
    core = lax.axis_index("dp")
    keep_ref[...] = whole_ref[:, pl.ds(pl.multiple_of(core * half, half), half)]
    send_ref[...] = whole_ref[:, pl.ds(pl.multiple_of((1 - core) * half, half), half)]


def keyval_kernel(mine_ref, theirs_ref, weight_ref, keep_ref, send_ref):
    rows = jnp.concatenate([mine_ref[...], theirs_ref[...]], axis=0)
    width = keep_ref.shape[1] // 2
    core = lax.axis_index("dp")
    for out_ref, owner in ((send_ref, 1 - core), (keep_ref, core)):
        for part in range(2):
            start = pl.multiple_of((part * 2 + owner) * width, width)
            out_ref[:, part * width : (part + 1) * width] = dot(
                rows, weight_ref[:, pl.ds(start, width)]
            )


def query_kernel(mine_ref, theirs_ref, weight_ref, keep_ref, send_ref):
    rows = jnp.concatenate([mine_ref[...], theirs_ref[...]], axis=0)
    width = keep_ref.shape[1]
    step = min(512, width)
    core = lax.axis_index("dp")
    for out_ref, owner in ((send_ref, 1 - core), (keep_ref, core)):
        for offset in range(0, width, step):
            start = pl.multiple_of(owner * width + offset, step)
            out_ref[:, offset : offset + step] = dot(rows, weight_ref[:, pl.ds(start, step)])


def summed(keep_ref, came_ref, columns):
    half = keep_ref.shape[0] // 2
    came = came_ref[:, columns]
    return keep_ref[:, columns] + jnp.concatenate([came[half:], came[:half]], axis=0)


def turned(vectors, cosine, sine):
    return vectors * cosine + pltpu.roll(vectors, HEAD_DIM // 2, 1) * sine


def keyval_turn_kernel(keep_ref, came_ref, cosine_ref, sine_ref, out_ref):
    width = out_ref.shape[1]
    for start in range(0, width, HEAD_DIM):
        columns = slice(start, start + HEAD_DIM)
        total = summed(keep_ref, came_ref, columns)
        if start < width // 2:
            total = turned(total, cosine_ref[...], sine_ref[...])
        out_ref[:, columns] = total.astype(bf16)


def query_turn_kernel(keep_ref, came_ref, cosine_ref, sine_ref, out_ref):
    for head in range(out_ref.shape[0]):
        columns = slice(head * HEAD_DIM, (head + 1) * HEAD_DIM)
        total = summed(keep_ref, came_ref, columns)
        out_ref[head] = turned(total, cosine_ref[...], sine_ref[...]).astype(bf16)


def attention_kernel(places, along, first, last, query_ref, *refs):
    refs = list(refs)
    keyval_refs = [refs.pop(0) for _ in places]
    before = [] if first else [refs.pop(0) for _ in range(3)]
    weight_ref = refs.pop(0) if last else None
    after = [refs.pop(0) for _ in range(2 if last else 3)]
    score_ref = refs.pop(0)
    context_ref = refs.pop(0) if last else None
    heads, rows, _ = query_ref.shape
    half = rows // 2
    shared = keyval_refs[0].shape[1] // (2 * HEAD_DIM)
    sharing = heads // shared
    core = lax.axis_index("dp")
    chip = lax.axis_index("expert")
    plane, place = chip // along, chip % along

    def position(shape, axis):
        row = lax.broadcasted_iota(jnp.int32, shape, axis)
        return jnp.where(core == 0, row, jnp.where(row < half, row + half, row - half))

    if first:
        own_visible = position((rows, rows), 1) <= position((rows, rows), 0)
    seen = []
    for back, turn in places:
        if back == 0:
            seen.append((place ^ turn) < place)
        else:
            seen.append(plane >= back)
    factor = HEAD_DIM ** (-0.5) * math.log2(math.e)

    def one_group(group, _):
        key_columns = pl.ds(pl.multiple_of(group * HEAD_DIM, HEAD_DIM), HEAD_DIM)
        value_columns = pl.ds(
            pl.multiple_of((shared + group) * HEAD_DIM, HEAD_DIM), HEAD_DIM
        )

        def one_head(member):
            head = group * sharing + member
            query = query_ref[head]
            highest = None
            for index, keyval_ref in enumerate(keyval_refs):
                score = lax.dot_general(
                    query,
                    keyval_ref[:, key_columns],
                    (((1,), (1,)), ((), ())),
                    preferred_element_type=f32,
                ) * factor
                own = first and index == 0
                if own:
                    score = jnp.where(own_visible, score, masked_score)
                score_ref[member, :, index * rows : (index + 1) * rows] = score
                most = score[:, :HEAD_DIM]
                for start in range(HEAD_DIM, rows, HEAD_DIM):
                    most = jnp.maximum(most, score[:, start : start + HEAD_DIM])
                if not own:
                    most = jnp.where(seen[index], most, masked_score)
                highest = most if highest is None else jnp.maximum(highest, most)
            highest = jnp.broadcast_to(
                jnp.max(highest, axis=-1, keepdims=True), (rows, HEAD_DIM)
            )
            if first:
                totals = jnp.zeros((rows, HEAD_DIM), f32)
                mixed = jnp.zeros((rows, HEAD_DIM), f32)
            else:
                earlier = before[0][head]
                highest = jnp.maximum(highest, earlier)
                shrink = jnp.exp2(earlier - highest)
                totals = before[1][head] * shrink
                mixed = before[2][head] * shrink
            for index, keyval_ref in enumerate(keyval_refs):
                ceiling = highest
                if not (first and index == 0):
                    ceiling = jnp.where(seen[index], highest, -masked_score)
                probs = []
                for start in range(index * rows, (index + 1) * rows, HEAD_DIM):
                    expo = jnp.exp2(score_ref[member, :, start : start + HEAD_DIM] - ceiling)
                    totals = totals + expo
                    probs.append(expo.astype(bf16))
                mixed = mixed + dot(jnp.concatenate(probs, axis=1), keyval_ref[:, value_columns])
            if last:
                total = jnp.sum(totals, axis=-1, keepdims=True)
                context_ref[head] = (mixed / total).astype(bf16)
            else:
                after[0][head] = highest
                after[1][head] = totals
                after[2][head] = mixed

        for member in range(sharing):
            one_head(member)
        return 0

    lax.fori_loop(0, shared, one_group, 0)

    if last:
        send_ref, keep_ref = after
        context = jnp.concatenate([context_ref[head] for head in range(heads)], axis=1)
        step = min(512, send_ref.shape[1])
        for start in range(0, send_ref.shape[1], step):
            columns = slice(start, start + step)
            out = dot(context, weight_ref[:, columns])
            keep_ref[:, columns] = out[:half]
            send_ref[:, columns] = out[half:].astype(bf16)


def as_columns(rows_ref):
    count = rows_ref.shape[1]
    same = (
        lax.broadcasted_iota(jnp.int32, (count, count), 0)
        == lax.broadcasted_iota(jnp.int32, (count, count), 1)
    )
    return lax.dot_general(
        same.astype(f32),
        rows_ref[...].astype(f32),
        (((1,), (1,)), ((), ())),
        precision=lax.Precision.HIGHEST,
        preferred_element_type=f32,
    )


def placed(choice, plane):
    rows = choice.shape[0]
    first, second = choice[:, 0:1], choice[:, 1:2]
    lane = lax.broadcasted_iota(jnp.int32, (rows, 128), 1)
    goes = jnp.zeros((rows, 128), jnp.bool_)
    for step in range(EXPERTS):
        expert = plane ^ step
        goes = goes | ((lane == step) & ((first == expert) | (second == expert)))
    earlier = (
        lax.broadcasted_iota(jnp.int32, (rows, rows), 1)
        < lax.broadcasted_iota(jnp.int32, (rows, rows), 0)
    )
    slots = dot(earlier.astype(bf16), goes.astype(bf16)).astype(jnp.int32)
    slots = jnp.where(goes, slots, -1)
    return [
        (lane[:, :ROWS] == slots[:, step : step + 1]).astype(bf16) for step in range(EXPERTS)
    ]


def pack_kernel(along, keep_ref, came_ref, tokens_ref, gain_ref, choice_ref, residual_ref, *out_refs):
    attention = keep_ref[...] + came_ref[...].astype(f32)
    residual = (tokens_ref[...].astype(f32) + attention).astype(bf16)
    residual_ref[...] = residual
    mixed_in = normalized(residual.astype(f32), gain_ref[...])
    plane = lax.axis_index("expert") // along
    choice = as_columns(choice_ref).astype(jnp.int32)
    for out_ref, routing in zip(out_refs, placed(choice, plane)):
        out_ref[...] = lax.dot_general(
            routing, mixed_in, (((0,), (0,)), ((), ())), preferred_element_type=f32
        ).astype(bf16)


def fetch_kernel(parts, from_ref, to_ref, sem):
    rows = from_ref.shape[0] // parts
    copies = []
    for part in range(parts):
        block = pl.ds(part * rows, rows)
        copies.append(
            pltpu.make_async_copy(from_ref.at[block], to_ref.at[block], sem.at[part])
        )
    for copy in copies:
        copy.start()
    for copy in copies:
        copy.wait()


def fetched(weight):
    parts = 4
    return pl.pallas_call(
        functools.partial(fetch_kernel, parts),
        out_shape=jax.ShapeDtypeStruct(weight.shape, weight.dtype),
        in_specs=[pl.BlockSpec(memory_space=pltpu.HBM)],
        out_specs=VMEM,
        scratch_shapes=[pltpu.SemaphoreType.DMA((parts,))],
        compiler_params=pltpu.CompilerParams(vmem_limit_bytes=2 << 20),
        cost_estimate=pl.CostEstimate(
            flops=0, bytes_accessed=4 * weight.size, transcendentals=0
        ),
        name="fetch",
    )(weight)


def expert_kernel(count, gate_ref, up_ref, down_ref, *refs):
    row_refs, out_refs, hidden_ref = refs[:count], refs[count : 2 * count], refs[2 * count]
    rows = jnp.concatenate([row_ref[...] for row_ref in row_refs], axis=0)
    for start in range(0, hidden_ref.shape[1], HIDDEN_STEP):
        columns = slice(start, start + HIDDEN_STEP)
        gate = dot(rows, gate_ref[:, columns])
        upward = dot(rows, up_ref[:, columns])
        hidden_ref[:, columns] = (gate / (1.0 + jnp.exp(-gate)) * upward).astype(bf16)
    hidden = hidden_ref[...]
    for start in range(0, down_ref.shape[1], DOWN_STEP):
        columns = slice(start, start + DOWN_STEP)
        out = dot(hidden, down_ref[:, columns]).astype(bf16)
        for index, out_ref in enumerate(out_refs):
            out_ref[:, columns] = out[index * ROWS : (index + 1) * ROWS]


def experts(rows, expert_gate, expert_up, expert_down):
    width, hidden = expert_gate.shape
    count = len(rows)
    return call(
        functools.partial(expert_kernel, count),
        [jax.ShapeDtypeStruct((ROWS, width), bf16)] * count,
        (expert_gate, expert_up, expert_down, *rows),
        scratch=[pltpu.VMEM((count * ROWS, hidden), bf16)],
        flops=6 * count * ROWS * width * hidden,
        moved=6 * width * hidden,
        limit=12 << 20,
    )


def early_kernel(along, early, late, base_ref, choice_ref, weight_ref, *refs):
    refs = list(refs)
    row_refs = [refs.pop(0) for _ in early]
    out_ref = refs.pop(0)
    plane = lax.axis_index("expert") // along
    choice = as_columns(choice_ref).astype(jnp.int32)
    weights = as_columns(weight_ref)
    total = base_ref[...].astype(f32)
    routings = placed(choice, plane)

    def weight(step):
        return jnp.sum(jnp.where(choice == (plane ^ step), weights, 0.0), axis=1, keepdims=True)

    for step, row_ref in zip(early, row_refs):
        total = total + weight(step) * dot(routings[step], row_ref[...])
    out_ref[...] = total
    for index, step in enumerate(late):
        refs[2 * index][...] = routings[step]
        refs[2 * index + 1][...] = jnp.broadcast_to(weight(step), refs[2 * index + 1].shape)


def late_kernel(base_ref, *refs):
    total_ref, out_ref = base_ref, refs[-1]
    width = 128
    for start in range(0, out_ref.shape[1], 4 * width):
        columns = slice(start, start + 4 * width)
        total = total_ref[:, columns]
        for index in range(0, len(refs) - 1, 3):
            routing_ref, weight_ref, row_ref = refs[index : index + 3]
            weight = jnp.concatenate([weight_ref[...]] * 4, axis=1)
            total = total + weight * dot(routing_ref[...], row_ref[:, columns])
        out_ref[:, columns] = total.astype(out_ref.dtype)


def add(*terms):
    return sum(term.astype(f32) for term in terms).astype(bf16)


def body(
    tokens,
    expert_choice,
    gate_weights,
    attention_gain,
    query_weight,
    key_value_weight,
    output_weight,
    feedforward_gain,
    expert_gate,
    expert_up,
    expert_down,
):
    local_rows, model_width = tokens.shape
    share = query_weight.shape[0]
    cores = lax.axis_size("dp")
    chips = lax.axis_size("expert")
    along = chips // EXPERTS
    query_width = query_weight.shape[1] // cores
    keyval_width = key_value_weight.shape[1] // cores
    heads = query_width // HEAD_DIM
    sharing = query_weight.shape[1] * 2 // key_value_weight.shape[1]
    pair_rows = local_rows * cores
    chip = lax.axis_index("expert")
    core = lax.axis_index("dp")

    def across(x):
        return lax.ppermute(x, "dp", [(i, i ^ 1) for i in range(cores)])

    def beside(x, turn):
        return lax.ppermute(x, "expert", [(i, i ^ turn) for i in range(chips)])

    def upward(x):
        return lax.ppermute(x, "expert", [(i, (i + along) % chips) for i in range(chips)])

    def planes(x, step):
        return lax.ppermute(x, "expert", [(i, i ^ (step * along)) for i in range(chips)])

    order = jnp.arange(pair_rows, dtype=jnp.int32)
    order = (order + core * local_rows) % pair_rows
    positions = chip * pair_rows + order
    halfway = HEAD_DIM // 2
    powers = jnp.arange(halfway, dtype=f32) * (2.0 / HEAD_DIM)
    inverse = base_theta ** (-powers)
    angles = positions.astype(f32)[:, None] * inverse[None, :]
    cosine, sine = jnp.cos(angles), jnp.sin(angles)
    cosine = jnp.concatenate([cosine, cosine], axis=1)
    sine = jnp.concatenate([-sine, sine], axis=1)

    shape = jax.ShapeDtypeStruct
    mine, outgoing = call(
        norm_kernel,
        [shape((local_rows, share), bf16)] * 2,
        (tokens, attention_gain.reshape(1, -1)),
        scratch=[pltpu.VMEM((local_rows, model_width), bf16)],
        flops=8 * local_rows * model_width,
        moved=4 * local_rows * model_width,
    )
    theirs = across(outgoing)
    key_value_weight = fetched(key_value_weight)
    keyval_keep, keyval_send = call(
        keyval_kernel,
        [shape((pair_rows, keyval_width), f32)] * 2,
        (mine, theirs, key_value_weight),
        flops=4 * pair_rows * share * keyval_width,
        moved=4 * share * keyval_width,
    )
    keyval_came = across(keyval_send)
    query_keep, query_send = call(
        query_kernel,
        [shape((pair_rows, query_width), f32)] * 2,
        (mine, theirs, query_weight),
        flops=4 * pair_rows * share * query_width,
        moved=4 * share * query_width,
    )
    query_came = across(query_send)
    keyval = call(
        keyval_turn_kernel,
        shape((pair_rows, keyval_width), bf16),
        (keyval_keep, keyval_came, cosine, sine),
        flops=8 * pair_rows * keyval_width,
        moved=10 * pair_rows * keyval_width,
    )
    queries = call(
        query_turn_kernel,
        shape((heads, pair_rows, HEAD_DIM), bf16),
        (query_keep, query_came, cosine, sine),
        flops=8 * pair_rows * query_width,
        moved=10 * pair_rows * query_width,
    )
    parts, part = [], []
    line = keyval
    for back in range(EXPERTS):
        if back:
            line = planes(line, 1) if back == EXPERTS - 1 else upward(line)
        part.append((line, (back, 0)))
        if back:
            parts.append(part)
            part = []
        part += [(beside(line, turn), (back, turn)) for turn in range(1, along)]
    parts.append(part)
    state = []
    for index, part in enumerate(parts):
        blocks, places = zip(*part) if part else ((), ())
        last = index == len(parts) - 1
        outs = [shape((heads, pair_rows, HEAD_DIM), f32)] * 3
        scratch = [
            pltpu.VMEM((sharing, pair_rows, pair_rows * max(1, len(blocks))), f32)
        ]
        if last:
            outs = [shape((local_rows, model_width), bf16), shape((local_rows, model_width), f32)]
            scratch.append(pltpu.VMEM((heads, pair_rows, HEAD_DIM), bf16))
        state = call(
            functools.partial(attention_kernel, places, along, index == 0, last),
            outs,
            (queries, *blocks, *state, *([output_weight] if last else [])),
            scratch=scratch,
            flops=4 * pair_rows * pair_rows * len(blocks) * query_width
            + 2 * pair_rows * query_width * model_width * last,
            moved=8 * pair_rows * query_width,
            limit=14 << 20,
        )
    attention_send, attention_keep = state
    attention_came = across(attention_send)
    residual, *packed = call(
        functools.partial(pack_kernel, along),
        [shape((local_rows, model_width), bf16)] + [shape((ROWS, model_width), bf16)] * EXPERTS,
        (
            attention_keep,
            attention_came,
            tokens,
            feedforward_gain.reshape(1, -1),
            expert_choice.T,
        ),
        flops=2 * EXPERTS * ROWS * local_rows * model_width,
        moved=12 * local_rows * model_width,
    )
    expert_gate = fetched(expert_gate)
    expert_up = fetched(expert_up)
    expert_down = fetched(expert_down)
    arrived = {}
    for step in ORDER:
        arrived[step] = planes(packed[step], step) if step else packed[step]
    collected = [None] * EXPERTS
    for step in ORDER:
        line = [arrived[step]] + [beside(arrived[step], turn) for turn in range(1, along)]
        line = line + [across(x) for x in line]
        outs = experts(line, expert_gate, expert_up, expert_down)
        others = [across(x) for x in outs[along:]]
        near = [add(own, other) for own, other in zip(outs[:along], others)]
        others = [beside(near[turn], turn) for turn in range(1, along)]
        reduced = add(near[0], *others)
        collected[step] = planes(reduced, step) if step else reduced
    a, b, c, d = ORDER
    early, late = (a, b), (c, d)
    prepared = [shape((local_rows, ROWS), bf16), shape((local_rows, 128), f32)] * len(late)
    total, *prepared = call(
        functools.partial(early_kernel, along, early, late),
        [shape((local_rows, model_width), f32), *prepared],
        (
            residual,
            expert_choice.T,
            gate_weights.T,
            *[collected[step] for step in early],
        ),
        flops=2 * len(early) * ROWS * local_rows * model_width,
        moved=8 * local_rows * model_width,
    )
    operands = [total]
    for index, step in enumerate(late):
        operands += [*prepared[2 * index : 2 * index + 2], collected[step]]
    return call(
        late_kernel,
        shape((local_rows, model_width), bf16),
        operands,
        flops=2 * len(late) * ROWS * local_rows * model_width,
        moved=8 * local_rows * model_width,
    )


def solution(mesh):
    assert mesh.shape["dp"] == 2 and mesh.shape["expert"] % EXPERTS == 0
    in_specs = (
        P(("group", "expert", "dp"), None),
        P(("group", "expert", "dp"), None),
        P(("group", "expert", "dp"), None),
        P(),
        P("dp", None),
        P("dp", None),
        P("dp", None),
        P(),
        P(None, ("expert", "dp")),
        P(None, ("expert", "dp")),
        P(("expert", "dp"), None),
    )
    out_specs = P(("group", "expert", "dp"), None)

    return jax.shard_map(body, mesh=mesh, in_specs=in_specs, out_specs=out_specs, check_vma=False)
```

```python
import functools
import math

import jax
import jax.numpy as jnp
from jax import lax
from jax.experimental import pallas as pl
from jax.experimental.pallas import tpu as pltpu
from jax.sharding import PartitionSpec as P


HEAD_DIM = 128
EXPERTS = 4
CAP = 70
ROWS = -(-CAP // 8) * 8

HIDDEN_STEP = 256
DOWN_STEP = 256
ORDER = (0, 2, 3, 1)

epsilon = 1e-05
base_theta = 1000000.0
masked_score = -1e30

VMEM = pl.BlockSpec(memory_space=pltpu.VMEM)
f32 = jnp.float32
bf16 = jnp.bfloat16


def dot(a, b):
    return jnp.dot(a, b, preferred_element_type=f32)


def call(kernel, outs, operands, scratch=(), flops=0, moved=0, limit=16 << 20):
    return pl.pallas_call(
        kernel,
        out_shape=outs,
        in_specs=[VMEM] * len(operands),
        out_specs=jax.tree.map(lambda _: VMEM, outs),
        scratch_shapes=list(scratch),
        compiler_params=pltpu.CompilerParams(vmem_limit_bytes=limit),
        cost_estimate=pl.CostEstimate(flops=flops, bytes_accessed=moved, transcendentals=0),
    )(*operands)


def normalized(widened, gain):
    spread = jnp.mean(widened * widened, axis=-1, keepdims=True)
    return (widened * lax.rsqrt(spread + epsilon) * gain).astype(bf16)


def norm_kernel(tokens_ref, gain_ref, keep_ref, send_ref, whole_ref):
    half = keep_ref.shape[1]
    whole_ref[...] = normalized(tokens_ref[...].astype(f32), gain_ref[...])
    core = lax.axis_index("dp")
    keep_ref[...] = whole_ref[:, pl.ds(pl.multiple_of(core * half, half), half)]
    send_ref[...] = whole_ref[:, pl.ds(pl.multiple_of((1 - core) * half, half), half)]


def keyval_kernel(mine_ref, theirs_ref, weight_ref, keep_ref, send_ref):
    rows = jnp.concatenate([mine_ref[...], theirs_ref[...]], axis=0)
    width = keep_ref.shape[1] // 2
    core = lax.axis_index("dp")
    for out_ref, owner in ((send_ref, 1 - core), (keep_ref, core)):
        for part in range(2):
            start = pl.multiple_of((part * 2 + owner) * width, width)
            out_ref[:, part * width : (part + 1) * width] = dot(
                rows, weight_ref[:, pl.ds(start, width)]
            )


def query_kernel(mine_ref, theirs_ref, weight_ref, keep_ref, send_ref):
    rows = jnp.concatenate([mine_ref[...], theirs_ref[...]], axis=0)
    width = keep_ref.shape[1]
    step = min(512, width)
    core = lax.axis_index("dp")
    for out_ref, owner in ((send_ref, 1 - core), (keep_ref, core)):
        for offset in range(0, width, step):
            start = pl.multiple_of(owner * width + offset, step)
            out_ref[:, offset : offset + step] = dot(rows, weight_ref[:, pl.ds(start, step)])


def summed(keep_ref, came_ref, columns):
    half = keep_ref.shape[0] // 2
    came = came_ref[:, columns]
    return keep_ref[:, columns] + jnp.concatenate([came[half:], came[:half]], axis=0)


def turned(vectors, cosine, sine):
    return vectors * cosine + pltpu.roll(vectors, HEAD_DIM // 2, 1) * sine


def keyval_turn_kernel(keep_ref, came_ref, cosine_ref, sine_ref, out_ref):
    width = out_ref.shape[1]
    for start in range(0, width, HEAD_DIM):
        columns = slice(start, start + HEAD_DIM)
        total = summed(keep_ref, came_ref, columns)
        if start < width // 2:
            total = turned(total, cosine_ref[...], sine_ref[...])
        out_ref[:, columns] = total.astype(bf16)


def query_turn_kernel(keep_ref, came_ref, cosine_ref, sine_ref, out_ref):
    for head in range(out_ref.shape[0]):
        columns = slice(head * HEAD_DIM, (head + 1) * HEAD_DIM)
        total = summed(keep_ref, came_ref, columns)
        out_ref[head] = turned(total, cosine_ref[...], sine_ref[...]).astype(bf16)


def attention_kernel(places, along, first, last, query_ref, *refs):
    refs = list(refs)
    keyval_refs = [refs.pop(0) for _ in places]
    before = [] if first else [refs.pop(0) for _ in range(3)]
    weight_ref = refs.pop(0) if last else None
    after = [refs.pop(0) for _ in range(2 if last else 3)]
    score_ref = refs.pop(0)
    context_ref = refs.pop(0) if last else None
    heads, rows, _ = query_ref.shape
    half = rows // 2
    shared = keyval_refs[0].shape[1] // (2 * HEAD_DIM)
    sharing = heads // shared
    core = lax.axis_index("dp")
    chip = lax.axis_index("expert")
    plane, place = chip // along, chip % along

    def position(shape, axis):
        row = lax.broadcasted_iota(jnp.int32, shape, axis)
        return jnp.where(core == 0, row, jnp.where(row < half, row + half, row - half))

    if first:
        own_visible = position((rows, rows), 1) <= position((rows, rows), 0)
    seen = []
    for back, turn in places:
        if back == 0:
            seen.append((place ^ turn) < place)
        else:
            seen.append(plane >= back)
    factor = HEAD_DIM ** (-0.5) * math.log2(math.e)

    def one_group(group, _):
        key_columns = pl.ds(pl.multiple_of(group * HEAD_DIM, HEAD_DIM), HEAD_DIM)
        value_columns = pl.ds(
            pl.multiple_of((shared + group) * HEAD_DIM, HEAD_DIM), HEAD_DIM
        )

        def one_head(member):
            head = group * sharing + member
            query = query_ref[head]
            highest = None
            for index, keyval_ref in enumerate(keyval_refs):
                score = lax.dot_general(
                    query,
                    keyval_ref[:, key_columns],
                    (((1,), (1,)), ((), ())),
                    preferred_element_type=f32,
                ) * factor
                own = first and index == 0
                if own:
                    score = jnp.where(own_visible, score, masked_score)
                score_ref[member, :, index * rows : (index + 1) * rows] = score
                most = score[:, :HEAD_DIM]
                for start in range(HEAD_DIM, rows, HEAD_DIM):
                    most = jnp.maximum(most, score[:, start : start + HEAD_DIM])
                if not own:
                    most = jnp.where(seen[index], most, masked_score)
                highest = most if highest is None else jnp.maximum(highest, most)
            highest = jnp.broadcast_to(
                jnp.max(highest, axis=-1, keepdims=True), (rows, HEAD_DIM)
            )
            if first:
                totals = jnp.zeros((rows, HEAD_DIM), f32)
                mixed = jnp.zeros((rows, HEAD_DIM), f32)
            else:
                earlier = before[0][head]
                highest = jnp.maximum(highest, earlier)
                shrink = jnp.exp2(earlier - highest)
                totals = before[1][head] * shrink
                mixed = before[2][head] * shrink
            for index, keyval_ref in enumerate(keyval_refs):
                ceiling = highest
                if not (first and index == 0):
                    ceiling = jnp.where(seen[index], highest, -masked_score)
                probs = []
                for start in range(index * rows, (index + 1) * rows, HEAD_DIM):
                    expo = jnp.exp2(score_ref[member, :, start : start + HEAD_DIM] - ceiling)
                    totals = totals + expo
                    probs.append(expo.astype(bf16))
                mixed = mixed + dot(jnp.concatenate(probs, axis=1), keyval_ref[:, value_columns])
            if last:
                total = jnp.sum(totals, axis=-1, keepdims=True)
                context_ref[head] = (mixed / total).astype(bf16)
            else:
                after[0][head] = highest
                after[1][head] = totals
                after[2][head] = mixed

        for member in range(sharing):
            one_head(member)
        return 0

    lax.fori_loop(0, shared, one_group, 0)

    if last:
        send_ref, keep_ref = after
        context = jnp.concatenate([context_ref[head] for head in range(heads)], axis=1)
        step = min(512, send_ref.shape[1])
        for start in range(0, send_ref.shape[1], step):
            columns = slice(start, start + step)
            out = dot(context, weight_ref[:, columns])
            keep_ref[:, columns] = out[:half]
            send_ref[:, columns] = out[half:].astype(bf16)


def as_columns(rows_ref):
    count = rows_ref.shape[1]
    same = (
        lax.broadcasted_iota(jnp.int32, (count, count), 0)
        == lax.broadcasted_iota(jnp.int32, (count, count), 1)
    )
    return lax.dot_general(
        same.astype(f32),
        rows_ref[...].astype(f32),
        (((1,), (1,)), ((), ())),
        precision=lax.Precision.HIGHEST,
        preferred_element_type=f32,
    )


def placed(choice, plane):
    rows = choice.shape[0]
    first, second = choice[:, 0:1], choice[:, 1:2]
    lane = lax.broadcasted_iota(jnp.int32, (rows, 128), 1)
    goes = jnp.zeros((rows, 128), jnp.bool_)
    for step in range(EXPERTS):
        expert = plane ^ step
        goes = goes | ((lane == step) & ((first == expert) | (second == expert)))
    earlier = (
        lax.broadcasted_iota(jnp.int32, (rows, rows), 1)
        < lax.broadcasted_iota(jnp.int32, (rows, rows), 0)
    )
    slots = dot(earlier.astype(bf16), goes.astype(bf16)).astype(jnp.int32)
    slots = jnp.where(goes, slots, -1)
    return [
        (lane[:, :ROWS] == slots[:, step : step + 1]).astype(bf16) for step in range(EXPERTS)
    ]


def route_kernel(along, choice_ref, weight_ref, *out_refs):
    plane = lax.axis_index("expert") // along
    choice = as_columns(choice_ref).astype(jnp.int32)
    weights = as_columns(weight_ref)
    for step, routing in enumerate(placed(choice, plane)):
        weight = jnp.where(choice == (plane ^ step), weights, 0.0)
        out_refs[2 * step][...] = routing
        out_refs[2 * step + 1][...] = jnp.broadcast_to(
            jnp.sum(weight, axis=1, keepdims=True), out_refs[2 * step + 1].shape
        )


def pack_kernel(keep_ref, came_ref, tokens_ref, gain_ref, *refs):
    routing_refs, residual_ref, out_refs = refs[:EXPERTS], refs[EXPERTS], refs[EXPERTS + 1 :]
    attention = keep_ref[...] + came_ref[...].astype(f32)
    residual = (tokens_ref[...].astype(f32) + attention).astype(bf16)
    residual_ref[...] = residual
    mixed_in = normalized(residual.astype(f32), gain_ref[...])
    for routing_ref, out_ref in zip(routing_refs, out_refs):
        out_ref[...] = lax.dot_general(
            routing_ref[...], mixed_in, (((0,), (0,)), ((), ())), preferred_element_type=f32
        ).astype(bf16)


def fetch_kernel(parts, from_ref, to_ref, sem):
    rows = from_ref.shape[0] // parts
    copies = []
    for part in range(parts):
        block = pl.ds(part * rows, rows)
        copies.append(
            pltpu.make_async_copy(from_ref.at[block], to_ref.at[block], sem.at[part])
        )
    for copy in copies:
        copy.start()
    for copy in copies:
        copy.wait()


def fetched(weight):
    parts = 4
    return pl.pallas_call(
        functools.partial(fetch_kernel, parts),
        out_shape=jax.ShapeDtypeStruct(weight.shape, weight.dtype),
        in_specs=[pl.BlockSpec(memory_space=pltpu.HBM)],
        out_specs=VMEM,
        scratch_shapes=[pltpu.SemaphoreType.DMA((parts,))],
        compiler_params=pltpu.CompilerParams(vmem_limit_bytes=2 << 20),
        cost_estimate=pl.CostEstimate(
            flops=0, bytes_accessed=4 * weight.size, transcendentals=0
        ),
        name="fetch",
    )(weight)


def expert_kernel(count, gate_ref, up_ref, down_ref, *refs):
    row_refs, out_refs, hidden_ref = refs[:count], refs[count : 2 * count], refs[2 * count]
    rows = jnp.concatenate([row_ref[...] for row_ref in row_refs], axis=0)
    for start in range(0, hidden_ref.shape[1], HIDDEN_STEP):
        columns = slice(start, start + HIDDEN_STEP)
        gate = dot(rows, gate_ref[:, columns])
        upward = dot(rows, up_ref[:, columns])
        hidden_ref[:, columns] = (gate / (1.0 + jnp.exp(-gate)) * upward).astype(bf16)
    hidden = hidden_ref[...]
    for start in range(0, down_ref.shape[1], DOWN_STEP):
        columns = slice(start, start + DOWN_STEP)
        out = dot(hidden, down_ref[:, columns]).astype(bf16)
        for index, out_ref in enumerate(out_refs):
            out_ref[:, columns] = out[index * ROWS : (index + 1) * ROWS]


def experts(rows, expert_gate, expert_up, expert_down):
    width, hidden = expert_gate.shape
    count = len(rows)
    return call(
        functools.partial(expert_kernel, count),
        [jax.ShapeDtypeStruct((ROWS, width), bf16)] * count,
        (expert_gate, expert_up, expert_down, *rows),
        scratch=[pltpu.VMEM((count * ROWS, hidden), bf16)],
        flops=6 * count * ROWS * width * hidden,
        moved=6 * width * hidden,
        limit=12 << 20,
    )


def combine_kernel(base_ref, *refs):
    total_ref, out_ref = base_ref, refs[-1]
    width = 128
    for start in range(0, out_ref.shape[1], 4 * width):
        columns = slice(start, start + 4 * width)
        total = total_ref[:, columns].astype(f32)
        for index in range(0, len(refs) - 1, 3):
            routing_ref, weight_ref, row_ref = refs[index : index + 3]
            weight = jnp.concatenate([weight_ref[...]] * 4, axis=1)
            total = total + weight * dot(routing_ref[...], row_ref[:, columns])
        out_ref[:, columns] = total.astype(out_ref.dtype)


def add(*terms):
    return sum(term.astype(f32) for term in terms).astype(bf16)


def body(
    tokens,
    expert_choice,
    gate_weights,
    attention_gain,
    query_weight,
    key_value_weight,
    output_weight,
    feedforward_gain,
    expert_gate,
    expert_up,
    expert_down,
):
    local_rows, model_width = tokens.shape
    share = query_weight.shape[0]
    cores = lax.axis_size("dp")
    chips = lax.axis_size("expert")
    along = chips // EXPERTS
    query_width = query_weight.shape[1] // cores
    keyval_width = key_value_weight.shape[1] // cores
    heads = query_width // HEAD_DIM
    sharing = query_weight.shape[1] * 2 // key_value_weight.shape[1]
    pair_rows = local_rows * cores
    chip = lax.axis_index("expert")
    core = lax.axis_index("dp")

    def across(x):
        return lax.ppermute(x, "dp", [(i, i ^ 1) for i in range(cores)])

    def beside(x, turn):
        return lax.ppermute(x, "expert", [(i, i ^ turn) for i in range(chips)])

    def upward(x):
        return lax.ppermute(x, "expert", [(i, (i + along) % chips) for i in range(chips)])

    def planes(x, step):
        return lax.ppermute(x, "expert", [(i, i ^ (step * along)) for i in range(chips)])

    order = jnp.arange(pair_rows, dtype=jnp.int32)
    order = (order + core * local_rows) % pair_rows
    positions = chip * pair_rows + order
    halfway = HEAD_DIM // 2
    powers = jnp.arange(halfway, dtype=f32) * (2.0 / HEAD_DIM)
    inverse = base_theta ** (-powers)
    angles = positions.astype(f32)[:, None] * inverse[None, :]
    cosine, sine = jnp.cos(angles), jnp.sin(angles)
    cosine = jnp.concatenate([cosine, cosine], axis=1)
    sine = jnp.concatenate([-sine, sine], axis=1)

    shape = jax.ShapeDtypeStruct
    mine, outgoing = call(
        norm_kernel,
        [shape((local_rows, share), bf16)] * 2,
        (tokens, attention_gain.reshape(1, -1)),
        scratch=[pltpu.VMEM((local_rows, model_width), bf16)],
        flops=8 * local_rows * model_width,
        moved=4 * local_rows * model_width,
    )
    theirs = across(outgoing)
    key_value_weight = fetched(key_value_weight)
    keyval_keep, keyval_send = call(
        keyval_kernel,
        [shape((pair_rows, keyval_width), f32)] * 2,
        (mine, theirs, key_value_weight),
        flops=4 * pair_rows * share * keyval_width,
        moved=4 * share * keyval_width,
    )
    keyval_came = across(keyval_send)
    query_keep, query_send = call(
        query_kernel,
        [shape((pair_rows, query_width), f32)] * 2,
        (mine, theirs, query_weight),
        flops=4 * pair_rows * share * query_width,
        moved=4 * share * query_width,
    )
    query_came = across(query_send)
    keyval = call(
        keyval_turn_kernel,
        shape((pair_rows, keyval_width), bf16),
        (keyval_keep, keyval_came, cosine, sine),
        flops=8 * pair_rows * keyval_width,
        moved=10 * pair_rows * keyval_width,
    )
    queries = call(
        query_turn_kernel,
        shape((heads, pair_rows, HEAD_DIM), bf16),
        (query_keep, query_came, cosine, sine),
        flops=8 * pair_rows * query_width,
        moved=10 * pair_rows * query_width,
    )
    parts, part = [], []
    line = keyval
    for back in range(EXPERTS):
        if back:
            line = planes(line, 1) if back == EXPERTS - 1 else upward(line)
        part.append((line, (back, 0)))
        if back:
            parts.append(part)
            part = []
        part += [(beside(line, turn), (back, turn)) for turn in range(1, along)]
    parts.append(part)
    state = []
    for index, part in enumerate(parts):
        blocks, places = zip(*part) if part else ((), ())
        last = index == len(parts) - 1
        outs = [shape((heads, pair_rows, HEAD_DIM), f32)] * 3
        scratch = [
            pltpu.VMEM((sharing, pair_rows, pair_rows * max(1, len(blocks))), f32)
        ]
        if last:
            outs = [shape((local_rows, model_width), bf16), shape((local_rows, model_width), f32)]
            scratch.append(pltpu.VMEM((heads, pair_rows, HEAD_DIM), bf16))
        state = call(
            functools.partial(attention_kernel, places, along, index == 0, last),
            outs,
            (queries, *blocks, *state, *([output_weight] if last else [])),
            scratch=scratch,
            flops=4 * pair_rows * pair_rows * len(blocks) * query_width
            + 2 * pair_rows * query_width * model_width * last,
            moved=8 * pair_rows * query_width,
            limit=14 << 20,
        )
    attention_send, attention_keep = state
    attention_came = across(attention_send)
    routes = [shape((local_rows, ROWS), bf16), shape((local_rows, 128), f32)] * EXPERTS
    routes = call(
        functools.partial(route_kernel, along),
        routes,
        (expert_choice.T, gate_weights.T),
        flops=4 * local_rows * local_rows * 128,
        moved=4 * EXPERTS * local_rows * 256,
    )
    residual, *packed = call(
        pack_kernel,
        [shape((local_rows, model_width), bf16)] + [shape((ROWS, model_width), bf16)] * EXPERTS,
        (
            attention_keep,
            attention_came,
            tokens,
            feedforward_gain.reshape(1, -1),
            *routes[::2],
        ),
        flops=2 * EXPERTS * ROWS * local_rows * model_width,
        moved=12 * local_rows * model_width,
    )
    expert_gate = fetched(expert_gate)
    expert_up = fetched(expert_up)
    expert_down = fetched(expert_down)
    arrived = {}
    for step in ORDER:
        arrived[step] = planes(packed[step], step) if step else packed[step]
    collected = [None] * EXPERTS
    for step in ORDER:
        line = [arrived[step]] + [beside(arrived[step], turn) for turn in range(1, along)]
        line = line + [across(x) for x in line]
        outs = experts(line, expert_gate, expert_up, expert_down)
        others = [across(x) for x in outs[along:]]
        near = [add(own, other) for own, other in zip(outs[:along], others)]
        others = [beside(near[turn], turn) for turn in range(1, along)]
        reduced = add(near[0], *others)
        collected[step] = planes(reduced, step) if step else reduced
    a, b, c, d = ORDER
    early, late = (a, b), (c, d)

    def combined(base, steps, kind):
        operands = [base]
        for step in steps:
            operands += [*routes[2 * step : 2 * step + 2], collected[step]]
        return call(
            combine_kernel,
            shape((local_rows, model_width), kind),
            operands,
            flops=2 * len(steps) * ROWS * local_rows * model_width,
            moved=8 * local_rows * model_width,
        )

    total = combined(residual, early, f32)
    return combined(total, late, bf16)


def solution(mesh):
    assert mesh.shape["dp"] == 2 and mesh.shape["expert"] % EXPERTS == 0
    in_specs = (
        P(("group", "expert", "dp"), None),
        P(("group", "expert", "dp"), None),
        P(("group", "expert", "dp"), None),
        P(),
        P("dp", None),
        P("dp", None),
        P("dp", None),
        P(),
        P(None, ("expert", "dp")),
        P(None, ("expert", "dp")),
        P(("expert", "dp"), None),
    )
    out_specs = P(("group", "expert", "dp"), None)

    return jax.shard_map(body, mesh=mesh, in_specs=in_specs, out_specs=out_specs, check_vma=False)
```

```python
import functools
import math

import jax
import jax.numpy as jnp
from jax import lax
from jax.experimental import pallas as pl
from jax.experimental.pallas import tpu as pltpu
from jax.sharding import PartitionSpec as P


HEAD_DIM = 128
EXPERTS = 4
CAP = 70
ROWS = -(-CAP // 8) * 8

HIDDEN_STEP = 256
DOWN_STEP = 256
ORDER = (0, 2, 3, 1)

epsilon = 1e-05
base_theta = 1000000.0
masked_score = -1e30

VMEM = pl.BlockSpec(memory_space=pltpu.VMEM)
f32 = jnp.float32
bf16 = jnp.bfloat16


def dot(a, b):
    return jnp.dot(a, b, preferred_element_type=f32)


def call(kernel, outs, operands, scratch=(), flops=0, moved=0, limit=16 << 20):
    return pl.pallas_call(
        kernel,
        out_shape=outs,
        in_specs=[VMEM] * len(operands),
        out_specs=jax.tree.map(lambda _: VMEM, outs),
        scratch_shapes=list(scratch),
        compiler_params=pltpu.CompilerParams(vmem_limit_bytes=limit),
        cost_estimate=pl.CostEstimate(flops=flops, bytes_accessed=moved, transcendentals=0),
    )(*operands)


def normalized(widened, gain):
    spread = jnp.mean(widened * widened, axis=-1, keepdims=True)
    return (widened * lax.rsqrt(spread + epsilon) * gain).astype(bf16)


def norm_kernel(tokens_ref, gain_ref, keep_ref, send_ref, whole_ref):
    half = keep_ref.shape[1]
    whole_ref[...] = normalized(tokens_ref[...].astype(f32), gain_ref[...])
    core = lax.axis_index("dp")
    keep_ref[...] = whole_ref[:, pl.ds(pl.multiple_of(core * half, half), half)]
    send_ref[...] = whole_ref[:, pl.ds(pl.multiple_of((1 - core) * half, half), half)]


def keyval_kernel(mine_ref, theirs_ref, weight_ref, keep_ref, send_ref):
    rows = jnp.concatenate([mine_ref[...], theirs_ref[...]], axis=0)
    width = keep_ref.shape[1] // 2
    core = lax.axis_index("dp")
    for out_ref, owner in ((send_ref, 1 - core), (keep_ref, core)):
        for part in range(2):
            start = pl.multiple_of((part * 2 + owner) * width, width)
            out_ref[:, part * width : (part + 1) * width] = dot(
                rows, weight_ref[:, pl.ds(start, width)]
            )


def query_kernel(mine_ref, theirs_ref, weight_ref, keep_ref, send_ref):
    rows = jnp.concatenate([mine_ref[...], theirs_ref[...]], axis=0)
    width = keep_ref.shape[1]
    step = min(512, width)
    core = lax.axis_index("dp")
    for out_ref, owner in ((send_ref, 1 - core), (keep_ref, core)):
        for offset in range(0, width, step):
            start = pl.multiple_of(owner * width + offset, step)
            out_ref[:, offset : offset + step] = dot(rows, weight_ref[:, pl.ds(start, step)])


def summed(keep_ref, came_ref, columns):
    half = keep_ref.shape[0] // 2
    came = came_ref[:, columns]
    return keep_ref[:, columns] + jnp.concatenate([came[half:], came[:half]], axis=0)


def turned(vectors, cosine, sine):
    return vectors * cosine + pltpu.roll(vectors, HEAD_DIM // 2, 1) * sine


def keyval_turn_kernel(keep_ref, came_ref, cosine_ref, sine_ref, out_ref):
    width = out_ref.shape[1]
    for start in range(0, width, HEAD_DIM):
        columns = slice(start, start + HEAD_DIM)
        total = summed(keep_ref, came_ref, columns)
        if start < width // 2:
            total = turned(total, cosine_ref[...], sine_ref[...])
        out_ref[:, columns] = total.astype(bf16)


def query_turn_kernel(keep_ref, came_ref, cosine_ref, sine_ref, out_ref):
    for head in range(out_ref.shape[0]):
        columns = slice(head * HEAD_DIM, (head + 1) * HEAD_DIM)
        total = summed(keep_ref, came_ref, columns)
        out_ref[head] = turned(total, cosine_ref[...], sine_ref[...]).astype(bf16)


def attention_kernel(places, along, first, last, query_ref, *refs):
    refs = list(refs)
    keyval_refs = [refs.pop(0) for _ in places]
    before = [] if first else [refs.pop(0) for _ in range(3)]
    weight_ref = refs.pop(0) if last else None
    after = [refs.pop(0) for _ in range(2 if last else 3)]
    score_ref = refs.pop(0)
    context_ref = refs.pop(0) if last else None
    heads, rows, _ = query_ref.shape
    half = rows // 2
    shared = keyval_refs[0].shape[1] // (2 * HEAD_DIM)
    sharing = heads // shared
    core = lax.axis_index("dp")
    chip = lax.axis_index("expert")
    plane, place = chip // along, chip % along

    def position(shape, axis):
        row = lax.broadcasted_iota(jnp.int32, shape, axis)
        return jnp.where(core == 0, row, jnp.where(row < half, row + half, row - half))

    if first:
        own_visible = position((rows, rows), 1) <= position((rows, rows), 0)
    seen = []
    for back, turn in places:
        if back == 0:
            seen.append((place ^ turn) < place)
        else:
            seen.append(plane >= back)
    factor = HEAD_DIM ** (-0.5) * math.log2(math.e)

    def one_group(group, _):
        key_columns = pl.ds(pl.multiple_of(group * HEAD_DIM, HEAD_DIM), HEAD_DIM)
        value_columns = pl.ds(
            pl.multiple_of((shared + group) * HEAD_DIM, HEAD_DIM), HEAD_DIM
        )

        def one_head(member):
            head = group * sharing + member
            query = query_ref[head]
            highest = None
            for index, keyval_ref in enumerate(keyval_refs):
                score = lax.dot_general(
                    query,
                    keyval_ref[:, key_columns],
                    (((1,), (1,)), ((), ())),
                    preferred_element_type=f32,
                ) * factor
                own = first and index == 0
                if own:
                    score = jnp.where(own_visible, score, masked_score)
                score_ref[member, :, index * rows : (index + 1) * rows] = score
                most = score[:, :HEAD_DIM]
                for start in range(HEAD_DIM, rows, HEAD_DIM):
                    most = jnp.maximum(most, score[:, start : start + HEAD_DIM])
                if not own:
                    most = jnp.where(seen[index], most, masked_score)
                highest = most if highest is None else jnp.maximum(highest, most)
            highest = jnp.broadcast_to(
                jnp.max(highest, axis=-1, keepdims=True), (rows, HEAD_DIM)
            )
            if first:
                totals = jnp.zeros((rows, HEAD_DIM), f32)
                mixed = jnp.zeros((rows, HEAD_DIM), f32)
            else:
                earlier = before[0][head]
                highest = jnp.maximum(highest, earlier)
                shrink = jnp.exp2(earlier - highest)
                totals = before[1][head] * shrink
                mixed = before[2][head] * shrink
            for index, keyval_ref in enumerate(keyval_refs):
                ceiling = highest
                if not (first and index == 0):
                    ceiling = jnp.where(seen[index], highest, -masked_score)
                probs = []
                for start in range(index * rows, (index + 1) * rows, HEAD_DIM):
                    expo = jnp.exp2(score_ref[member, :, start : start + HEAD_DIM] - ceiling)
                    totals = totals + expo
                    probs.append(expo.astype(bf16))
                mixed = mixed + dot(jnp.concatenate(probs, axis=1), keyval_ref[:, value_columns])
            if last:
                total = jnp.sum(totals, axis=-1, keepdims=True)
                context_ref[head] = (mixed / total).astype(bf16)
            else:
                after[0][head] = highest
                after[1][head] = totals
                after[2][head] = mixed

        for member in range(sharing):
            one_head(member)
        return 0

    lax.fori_loop(0, shared, one_group, 0)

    if last:
        send_ref, keep_ref = after
        context = jnp.concatenate([context_ref[head] for head in range(heads)], axis=1)
        step = min(512, send_ref.shape[1])
        for start in range(0, send_ref.shape[1], step):
            columns = slice(start, start + step)
            out = dot(context, weight_ref[:, columns])
            keep_ref[:, columns] = out[:half]
            send_ref[:, columns] = out[half:].astype(bf16)


def as_columns(rows_ref):
    count = rows_ref.shape[1]
    same = (
        lax.broadcasted_iota(jnp.int32, (count, count), 0)
        == lax.broadcasted_iota(jnp.int32, (count, count), 1)
    )
    return lax.dot_general(
        same.astype(f32),
        rows_ref[...].astype(f32),
        (((1,), (1,)), ((), ())),
        precision=lax.Precision.HIGHEST,
        preferred_element_type=f32,
    )


def placed(choice, plane):
    rows = choice.shape[0]
    first, second = choice[:, 0:1], choice[:, 1:2]
    lane = lax.broadcasted_iota(jnp.int32, (rows, 128), 1)
    goes = jnp.zeros((rows, 128), jnp.bool_)
    for step in range(EXPERTS):
        expert = plane ^ step
        goes = goes | ((lane == step) & ((first == expert) | (second == expert)))
    earlier = (
        lax.broadcasted_iota(jnp.int32, (rows, rows), 1)
        < lax.broadcasted_iota(jnp.int32, (rows, rows), 0)
    )
    slots = dot(earlier.astype(bf16), goes.astype(bf16)).astype(jnp.int32)
    slots = jnp.where(goes, slots, -1)
    return [
        (lane[:, :ROWS] == slots[:, step : step + 1]).astype(bf16) for step in range(EXPERTS)
    ]


def route_kernel(along, choice_ref, weight_ref, *out_refs):
    plane = lax.axis_index("expert") // along
    choice = as_columns(choice_ref).astype(jnp.int32)
    weights = as_columns(weight_ref)
    for step, routing in enumerate(placed(choice, plane)):
        weight = jnp.where(choice == (plane ^ step), weights, 0.0)
        out_refs[2 * step][...] = routing
        out_refs[2 * step + 1][...] = jnp.broadcast_to(
            jnp.sum(weight, axis=1, keepdims=True), out_refs[2 * step + 1].shape
        )


def pack_kernel(keep_ref, came_ref, tokens_ref, gain_ref, *refs):
    routing_refs, residual_ref, out_refs = refs[:EXPERTS], refs[EXPERTS], refs[EXPERTS + 1 :]
    attention = keep_ref[...] + came_ref[...].astype(f32)
    residual = (tokens_ref[...].astype(f32) + attention).astype(bf16)
    residual_ref[...] = residual
    mixed_in = normalized(residual.astype(f32), gain_ref[...])
    for routing_ref, out_ref in zip(routing_refs, out_refs):
        out_ref[...] = lax.dot_general(
            routing_ref[...], mixed_in, (((0,), (0,)), ((), ())), preferred_element_type=f32
        ).astype(bf16)


def fetch_kernel(parts, from_ref, to_ref, sem):
    rows = from_ref.shape[0] // parts
    copies = []
    for part in range(parts):
        block = pl.ds(part * rows, rows)
        copies.append(
            pltpu.make_async_copy(from_ref.at[block], to_ref.at[block], sem.at[part])
        )
    for copy in copies:
        copy.start()
    for copy in copies:
        copy.wait()


def fetched(weight):
    parts = 4
    return pl.pallas_call(
        functools.partial(fetch_kernel, parts),
        out_shape=jax.ShapeDtypeStruct(weight.shape, weight.dtype),
        in_specs=[pl.BlockSpec(memory_space=pltpu.HBM)],
        out_specs=VMEM,
        scratch_shapes=[pltpu.SemaphoreType.DMA((parts,))],
        compiler_params=pltpu.CompilerParams(vmem_limit_bytes=2 << 20),
        cost_estimate=pl.CostEstimate(
            flops=0, bytes_accessed=4 * weight.size, transcendentals=0
        ),
        name="fetch",
    )(weight)


def expert_kernel(count, gate_ref, up_ref, down_ref, *refs):
    row_refs, out_refs, hidden_ref = refs[:count], refs[count : 2 * count], refs[2 * count]
    rows = jnp.concatenate([row_ref[...] for row_ref in row_refs], axis=0)
    for start in range(0, hidden_ref.shape[1], HIDDEN_STEP):
        columns = slice(start, start + HIDDEN_STEP)
        gate = dot(rows, gate_ref[:, columns])
        upward = dot(rows, up_ref[:, columns])
        hidden_ref[:, columns] = (gate / (1.0 + jnp.exp(-gate)) * upward).astype(bf16)
    hidden = hidden_ref[...]
    for start in range(0, down_ref.shape[1], DOWN_STEP):
        columns = slice(start, start + DOWN_STEP)
        out = dot(hidden, down_ref[:, columns]).astype(bf16)
        for index, out_ref in enumerate(out_refs):
            out_ref[:, columns] = out[index * ROWS : (index + 1) * ROWS]


def experts(rows, expert_gate, expert_up, expert_down):
    width, hidden = expert_gate.shape
    count = len(rows)
    return call(
        functools.partial(expert_kernel, count),
        [jax.ShapeDtypeStruct((ROWS, width), bf16)] * count,
        (expert_gate, expert_up, expert_down, *rows),
        scratch=[pltpu.VMEM((count * ROWS, hidden), bf16)],
        flops=6 * count * ROWS * width * hidden,
        moved=6 * width * hidden,
        limit=12 << 20,
    )


def combine_kernel(base_ref, *refs):
    total_ref, out_ref = base_ref, refs[-1]
    width = 128
    for start in range(0, out_ref.shape[1], 4 * width):
        columns = slice(start, start + 4 * width)
        total = total_ref[:, columns].astype(f32)
        for index in range(0, len(refs) - 1, 3):
            routing_ref, weight_ref, row_ref = refs[index : index + 3]
            weight = jnp.concatenate([weight_ref[...]] * 4, axis=1)
            total = total + weight * dot(routing_ref[...], row_ref[:, columns])
        out_ref[:, columns] = total.astype(out_ref.dtype)


def last_kernel(total_ref, *refs):
    refs = list(refs)
    sem = refs.pop()
    held_ref = refs.pop()
    out_ref = refs.pop()
    width = 128
    step = 4 * width
    copies = []
    for start in range(0, held_ref.shape[1], step):
        columns = slice(start, start + step)
        total = total_ref[:, columns].astype(f32)
        for index in range(0, len(refs), 3):
            routing_ref, weight_ref, row_ref = refs[index : index + 3]
            weight = jnp.concatenate([weight_ref[...]] * 4, axis=1)
            total = total + weight * dot(routing_ref[...], row_ref[:, columns])
        held_ref[:, columns] = total.astype(held_ref.dtype)
        block = pl.ds(start, step)
        copy = pltpu.make_async_copy(
            held_ref.at[:, block], out_ref.at[:, block], sem.at[start // step]
        )
        copy.start()
        copies.append(copy)
    for copy in copies:
        copy.wait()


def add(*terms):
    return sum(term.astype(f32) for term in terms).astype(bf16)


def body(
    tokens,
    expert_choice,
    gate_weights,
    attention_gain,
    query_weight,
    key_value_weight,
    output_weight,
    feedforward_gain,
    expert_gate,
    expert_up,
    expert_down,
):
    local_rows, model_width = tokens.shape
    share = query_weight.shape[0]
    cores = lax.axis_size("dp")
    chips = lax.axis_size("expert")
    along = chips // EXPERTS
    query_width = query_weight.shape[1] // cores
    keyval_width = key_value_weight.shape[1] // cores
    heads = query_width // HEAD_DIM
    sharing = query_weight.shape[1] * 2 // key_value_weight.shape[1]
    pair_rows = local_rows * cores
    chip = lax.axis_index("expert")
    core = lax.axis_index("dp")

    def across(x):
        return lax.ppermute(x, "dp", [(i, i ^ 1) for i in range(cores)])

    def beside(x, turn):
        return lax.ppermute(x, "expert", [(i, i ^ turn) for i in range(chips)])

    def upward(x):
        return lax.ppermute(x, "expert", [(i, (i + along) % chips) for i in range(chips)])

    def planes(x, step):
        return lax.ppermute(x, "expert", [(i, i ^ (step * along)) for i in range(chips)])

    order = jnp.arange(pair_rows, dtype=jnp.int32)
    order = (order + core * local_rows) % pair_rows
    positions = chip * pair_rows + order
    halfway = HEAD_DIM // 2
    powers = jnp.arange(halfway, dtype=f32) * (2.0 / HEAD_DIM)
    inverse = base_theta ** (-powers)
    angles = positions.astype(f32)[:, None] * inverse[None, :]
    cosine, sine = jnp.cos(angles), jnp.sin(angles)
    cosine = jnp.concatenate([cosine, cosine], axis=1)
    sine = jnp.concatenate([-sine, sine], axis=1)

    shape = jax.ShapeDtypeStruct
    mine, outgoing = call(
        norm_kernel,
        [shape((local_rows, share), bf16)] * 2,
        (tokens, attention_gain.reshape(1, -1)),
        scratch=[pltpu.VMEM((local_rows, model_width), bf16)],
        flops=8 * local_rows * model_width,
        moved=4 * local_rows * model_width,
    )
    theirs = across(outgoing)
    key_value_weight = fetched(key_value_weight)
    keyval_keep, keyval_send = call(
        keyval_kernel,
        [shape((pair_rows, keyval_width), f32)] * 2,
        (mine, theirs, key_value_weight),
        flops=4 * pair_rows * share * keyval_width,
        moved=4 * share * keyval_width,
    )
    keyval_came = across(keyval_send)
    query_keep, query_send = call(
        query_kernel,
        [shape((pair_rows, query_width), f32)] * 2,
        (mine, theirs, query_weight),
        flops=4 * pair_rows * share * query_width,
        moved=4 * share * query_width,
    )
    query_came = across(query_send)
    keyval = call(
        keyval_turn_kernel,
        shape((pair_rows, keyval_width), bf16),
        (keyval_keep, keyval_came, cosine, sine),
        flops=8 * pair_rows * keyval_width,
        moved=10 * pair_rows * keyval_width,
    )
    queries = call(
        query_turn_kernel,
        shape((heads, pair_rows, HEAD_DIM), bf16),
        (query_keep, query_came, cosine, sine),
        flops=8 * pair_rows * query_width,
        moved=10 * pair_rows * query_width,
    )
    parts, part = [], []
    line = keyval
    for back in range(EXPERTS):
        if back:
            line = planes(line, 1) if back == EXPERTS - 1 else upward(line)
        part.append((line, (back, 0)))
        if back:
            parts.append(part)
            part = []
        part += [(beside(line, turn), (back, turn)) for turn in range(1, along)]
    parts.append(part)
    state = []
    for index, part in enumerate(parts):
        blocks, places = zip(*part) if part else ((), ())
        last = index == len(parts) - 1
        outs = [shape((heads, pair_rows, HEAD_DIM), f32)] * 3
        scratch = [
            pltpu.VMEM((sharing, pair_rows, pair_rows * max(1, len(blocks))), f32)
        ]
        if last:
            outs = [shape((local_rows, model_width), bf16), shape((local_rows, model_width), f32)]
            scratch.append(pltpu.VMEM((heads, pair_rows, HEAD_DIM), bf16))
        state = call(
            functools.partial(attention_kernel, places, along, index == 0, last),
            outs,
            (queries, *blocks, *state, *([output_weight] if last else [])),
            scratch=scratch,
            flops=4 * pair_rows * pair_rows * len(blocks) * query_width
            + 2 * pair_rows * query_width * model_width * last,
            moved=8 * pair_rows * query_width,
            limit=14 << 20,
        )
    attention_send, attention_keep = state
    attention_came = across(attention_send)
    routes = [shape((local_rows, ROWS), bf16), shape((local_rows, 128), f32)] * EXPERTS
    routes = call(
        functools.partial(route_kernel, along),
        routes,
        (expert_choice.T, gate_weights.T),
        flops=4 * local_rows * local_rows * 128,
        moved=4 * EXPERTS * local_rows * 256,
    )
    residual, *packed = call(
        pack_kernel,
        [shape((local_rows, model_width), bf16)] + [shape((ROWS, model_width), bf16)] * EXPERTS,
        (
            attention_keep,
            attention_came,
            tokens,
            feedforward_gain.reshape(1, -1),
            *routes[::2],
        ),
        flops=2 * EXPERTS * ROWS * local_rows * model_width,
        moved=12 * local_rows * model_width,
    )
    expert_gate = fetched(expert_gate)
    expert_up = fetched(expert_up)
    expert_down = fetched(expert_down)
    arrived = {}
    for step in ORDER:
        arrived[step] = planes(packed[step], step) if step else packed[step]
    collected = [None] * EXPERTS
    for step in ORDER:
        line = [arrived[step]] + [beside(arrived[step], turn) for turn in range(1, along)]
        line = line + [across(x) for x in line]
        outs = experts(line, expert_gate, expert_up, expert_down)
        others = [across(x) for x in outs[along:]]
        near = [add(own, other) for own, other in zip(outs[:along], others)]
        others = [beside(near[turn], turn) for turn in range(1, along)]
        reduced = add(near[0], *others)
        collected[step] = planes(reduced, step) if step else reduced
    a, b, c, d = ORDER
    early, late = (a, b), (c, d)

    def combined(base, steps, kind, last=False):
        operands = [base]
        for step in steps:
            operands += [*routes[2 * step : 2 * step + 2], collected[step]]
        out = shape((local_rows, model_width), kind)
        if last:
            return pl.pallas_call(
                last_kernel,
                out_shape=out,
                in_specs=[VMEM] * len(operands),
                out_specs=pl.BlockSpec(memory_space=pl.ANY),
                scratch_shapes=[
                    pltpu.VMEM(out.shape, kind),
                    pltpu.SemaphoreType.DMA((model_width // 512,)),
                ],
                compiler_params=pltpu.CompilerParams(vmem_limit_bytes=16 << 20),
                name="combine",
            )(*operands)
        return call(
            combine_kernel,
            out,
            operands,
            flops=2 * len(steps) * ROWS * local_rows * model_width,
            moved=8 * local_rows * model_width,
        )

    total = combined(residual, early, f32)
    return combined(total, late, bf16, last=True)


def solution(mesh):
    assert mesh.shape["dp"] == 2 and mesh.shape["expert"] % EXPERTS == 0
    in_specs = (
        P(("group", "expert", "dp"), None),
        P(("group", "expert", "dp"), None),
        P(("group", "expert", "dp"), None),
        P(),
        P("dp", None),
        P("dp", None),
        P("dp", None),
        P(),
        P(None, ("expert", "dp")),
        P(None, ("expert", "dp")),
        P(("expert", "dp"), None),
    )
    out_specs = P(("group", "expert", "dp"), None)

    return jax.shard_map(body, mesh=mesh, in_specs=in_specs, out_specs=out_specs, check_vma=False)
```
